32 devices in a mesh: prow: 4 (over y, core), pcol: 8 (over z, x).
Axes of the slice: x: 2, y: 2, z: 4, core: 2. Of those that a mesh axis runs over, the one named last changes fastest.
Arguments:
- matrix_slab: float32 [2048, 2048], P('pcol', 'prow'), may hold values from -1024 to 1024
- contributions: float32 [4, 256, 64, 256], P('prow', 'pcol'), may hold values from -3 to 3
- target_column: int32 [4, 256], P('prow', 'pcol'), may hold values from 0 to 31, as said below
- target_rows: int32 [4, 256], P('prow', 'pcol'), may hold values from 0 to 1
- live_rows: int32 [4, 256], P('prow', 'pcol'), may hold values from 1 to 256
- pivot_index: int32 [1, 256], replicated, may hold values from 256 to 2047, as said below
Outputs:
- factored: float32 [2048, 2048], P('pcol', 'prow')
The draws below stay inside these ranges and needn't reach their ends.
Inputs may be any that keep to these rules, and one draw needn't show every extreme that they name: `pivot_index`: row k lists 256 distinct rows, each (k + 1) * 256 or more. `target_column`: of the 32 blocks held by one device, at most 8 have target column blocks within the columns of one index of pcol, and exactly 8 for some index.
All inputs are finite; a program needn't handle non-finite values.
Results may differ from the reference program's by a relative error of at most 0.0001.
Values sent between devices are 32-bit elements; how exact they have to be, the bound alone decides.
A program may use at most 128 MiB of HBM per device.

```python
import jax
import jax.numpy as jnp
from jax import lax

SLAB = 2048
PW = 256
PANELS = 1
NB = 64
TR = 256
CB_DEV = 32
ROWS_DEV = 512
COLS_DEV = 256
ROWS = 2048
MOST = 8
CB_ALL = 256
N_PROW = 4
N_PCOL = 8


def pivot_draw(key):
    pivot_list = []
    for panel_number in range(PANELS):
        offset = (panel_number + 1) * PW
        shuffled = jax.random.permutation(jax.random.fold_in(key, panel_number), ROWS - offset)
        pivot_list.append(shuffled[:PW] + offset)
    return jnp.stack(pivot_list).astype(jnp.int32)


def draw_pivot_index(key, part):
    return pivot_draw(jax.random.fold_in(key, 11))


def draw_matrix_slab(key, part):
    pivots = pivot_draw(jax.random.fold_in(key, 11))
    subkeys = jax.random.split(jax.random.fold_in(key, 23), 6)
    modest = jax.random.uniform(subkeys[0], (SLAB, ROWS), jnp.float32, -1.0, 1.0)
    strong = jax.random.uniform(subkeys[1], (SLAB, ROWS), jnp.float32, -1.0, 1.0) * PW
    initial = jnp.arange(ROWS, dtype=jnp.int32)
    already_used = jnp.zeros((ROWS,), jnp.bool_)
    pivot_marks = []
    holders = []
    for panel_number in range(PANELS):
        chosen = pivots[panel_number]
        source_rows = initial[chosen]
        already_used = already_used.at[source_rows].set(True)
        pivot_marks.append(already_used)
        holders.append(source_rows)
        panel_slots = jnp.arange(panel_number * PW, (panel_number + 1) * PW, dtype=jnp.int32)
        moved_out = initial[panel_slots]
        initial = initial.at[panel_slots].set(source_rows).at[chosen].set(moved_out)
    pivot_marks = jnp.stack(pivot_marks)
    column_panel = jnp.minimum(jnp.arange(SLAB) // PW, PANELS - 1)
    in_panels = (jnp.arange(SLAB) < PANELS * PW)[:, None]
    quiet_mask = jnp.logical_or(jnp.logical_not(in_panels), pivot_marks[column_panel])
    entries = jnp.where(quiet_mask, modest, strong)
    for panel_number in range(PANELS):
        panel_columns = panel_number * PW + jnp.arange(PW)
        block_entries = jax.random.uniform(jax.random.fold_in(subkeys[5], panel_number), (PW, PW), jnp.float32, -0.25 * PW, 0.25 * PW)
        entries = entries.at[panel_columns[:, None], holders[panel_number][None, :]].set(block_entries)
        sign_flip = jnp.where(jax.random.bernoulli(jax.random.fold_in(subkeys[2], panel_number), 0.5, (PW,)), 1.0, -1.0)
        magnitude = jax.random.uniform(jax.random.fold_in(subkeys[3], panel_number), (PW,), jnp.float32, 3.0 * PW, 4.0 * PW)
        entries = entries.at[panel_columns, holders[panel_number]].set(sign_flip * magnitude)
    return entries


def draw_target_column(key, part):
    local_blocks = COLS_DEV // NB

    def one_device(device_key):
        first_key, second_key, third_key, fourth_key = jax.random.split(device_key, 4)
        slot_owner = jnp.arange(N_PCOL * MOST, dtype=jnp.int32) // MOST
        busiest = jax.random.randint(first_key, (), 0, N_PCOL)
        others = jax.random.permutation(second_key, N_PCOL * MOST - MOST)[:CB_DEV - MOST] + MOST
        picked = jnp.concatenate([jnp.arange(MOST, dtype=jnp.int32), others.astype(jnp.int32)])
        owners = (slot_owner[picked] + busiest) % N_PCOL
        owners = owners[jax.random.permutation(third_key, CB_DEV)]
        within = jax.random.randint(fourth_key, (CB_DEV,), 0, local_blocks)
        return owners * local_blocks + within
    device_keys = jax.random.split(jax.random.fold_in(key, 31), N_PROW * N_PCOL)
    return jax.vmap(one_device)(device_keys).reshape(N_PROW, N_PCOL * CB_DEV).astype(jnp.int32)


def set_ends(values, own_key, low, high):
    longest = values.shape.index(max(values.shape))
    spots = []
    for shift in (0, 1):
        where = [jax.random.randint(jax.random.fold_in(own_key, axis), (), 0, length) for axis, length in enumerate(values.shape)]
        where[longest] = (where[longest] + shift) % values.shape[longest]
        spots.append(tuple(where))
    return values.at[spots[0]].set(low).at[spots[1]].set(high)


def shard_levels(key, shape, shards, low, largest):
    def one(dim, blocks):
        draws = jax.random.uniform(jax.random.fold_in(jax.random.fold_in(key, 6), dim), (blocks,), jnp.float32, low / len(shards), largest / len(shards))
        return jnp.repeat(jnp.exp(draws), shape[dim] // blocks).reshape((-1,) + (1,) * (len(shape) - dim - 1))

    level = one(*shards[0])
    for cut in shards[1:]:
        level = level * one(*cut)
    return level


def scatter_about(own_key, shape, scale, limit, cuts=(), kind=jnp.bfloat16):
    level = shard_levels(own_key, shape, cuts, -0.22, 0.18) if cuts else 1.0
    values = jax.random.normal(own_key, shape, jnp.float32) * scale * level
    return jnp.minimum(jnp.maximum(values, -limit), limit).astype(kind)


def setup_inputs(seed: int = 0) -> dict:
    keys = jax.random.split(jax.random.key(seed), 7)
    return {
        "matrix_slab": draw_matrix_slab(jax.random.fold_in(keys[6], 71), 0),
        "contributions": scatter_about(keys[1], (N_PROW, CB_ALL, NB, TR), 0.5, 3.0, ((0, 4), (1, 8)), jnp.float32),
        "target_column": draw_target_column(jax.random.fold_in(keys[6], 71), 0),
        "target_rows": set_ends(jax.random.randint(keys[3], (N_PROW, CB_ALL), 0, ROWS_DEV // TR), jax.random.fold_in(keys[3], 1), 0, (ROWS_DEV // TR) - 1).astype(jnp.int32),
        "live_rows": set_ends(jax.random.randint(keys[4], (N_PROW, CB_ALL), 1, TR + 1), jax.random.fold_in(keys[4], 1), 1, TR).astype(jnp.int32),
        "pivot_index": draw_pivot_index(jax.random.fold_in(keys[6], 71), 0),
    }


HIGHEST = lax.Precision.HIGHEST

def factor_block(square):
    extent = square.shape[0]
    if extent <= 16:
        for column in range(extent - 1):
            ratios = square[column + 1:, column] / square[column, column]
            square = square.at[column + 1:, column].set(ratios)
            square = square.at[column + 1:, column + 1:].add(-ratios[:, None] * square[column, column + 1:][None, :])
        return square
    middle = extent // 2
    top_left = factor_block(square[:middle, :middle])
    lower_unit = jnp.tril(top_left, -1) + jnp.eye(middle, dtype=square.dtype)
    upper_part = jnp.triu(top_left)
    right_part = jax.scipy.linalg.solve_triangular(lower_unit, square[:middle, middle:], lower=True, unit_diagonal=True)
    left_part = jax.scipy.linalg.solve_triangular(upper_part.T, square[middle:, :middle].T, lower=True).T
    schur_part = square[middle:, middle:] - jnp.dot(left_part, right_part, precision=HIGHEST)
    bottom = factor_block(schur_part)
    upper_half = jnp.concatenate([top_left, right_part], axis=1)
    lower_half = jnp.concatenate([left_part, bottom], axis=1)
    return jnp.concatenate([upper_half, lower_half], axis=0)

def split_factors(packed):
    extent = packed.shape[0]
    lower_unit = jnp.tril(packed, -1) + jnp.eye(extent, dtype=packed.dtype)
    return (lower_unit, jnp.triu(packed))

def reference(matrix_slab, contributions, target_column, target_rows, live_rows, pivot_index):
    blocks = contributions.reshape(N_PROW * CB_ALL, NB, TR)
    lengths = live_rows.reshape(-1)
    column_anchor = (target_column.reshape(-1) * NB).astype(jnp.int32)
    row_anchor = (jnp.arange(N_PROW, dtype=jnp.int32)[:, None] * ROWS_DEV + target_rows * TR).reshape(-1).astype(jnp.int32)
    positions = jnp.arange(TR, dtype=jnp.int32)

    def add_block(index, current):
        single = blocks[index] * (positions < lengths[index]).astype(blocks.dtype)[None, :]
        anchor = (column_anchor[index], row_anchor[index])
        window = lax.dynamic_slice(current, anchor, (NB, TR))
        return lax.dynamic_update_slice(current, window + single, anchor)
    matrix = lax.fori_loop(0, N_PROW * CB_ALL, add_block, matrix_slab)
    rows_all = jnp.arange(ROWS, dtype=jnp.int32)
    for panel_number in range(PANELS):
        panel_start = panel_number * PW
        panel_end = panel_start + PW
        chosen = pivot_index[panel_number]
        displaced = matrix[:, panel_start:panel_end]
        incoming = matrix[:, chosen]
        matrix = matrix.at[:, chosen].set(displaced)
        matrix = matrix.at[:, panel_start:panel_end].set(incoming)
        panel_cols = matrix[panel_start:panel_end, :]
        packed = factor_block(panel_cols[:, panel_start:panel_end].T)
        lower_unit, upper_part = split_factors(packed)
        lower_cols = jax.scipy.linalg.solve_triangular(upper_part.T, panel_cols, lower=True)
        upper_rows = jax.scipy.linalg.solve_triangular(lower_unit, matrix[:, panel_start:panel_end].T, lower=True, unit_diagonal=True)
        below_rows = rows_all >= panel_end
        renewed = panel_cols.at[:, panel_start:panel_end].set(packed.T)
        renewed = jnp.where(below_rows[None, :], lower_cols, renewed)
        trailing = upper_rows[:, panel_end:].T
        update = jnp.dot(trailing, lower_cols[:, panel_end:], precision=HIGHEST)
        matrix = matrix.at[panel_start:panel_end, :].set(renewed)
        matrix = matrix.at[panel_end:, panel_start:panel_end].set(trailing)
        matrix = matrix.at[panel_end:, panel_end:].add(-update)
    return matrix
```

```python
import functools

import jax
import jax.numpy as jnp
from jax import lax
from jax.experimental import pallas as pl
from jax.experimental.pallas import tpu as pltpu
from jax.sharding import PartitionSpec as P

PW = 256
NB = 64
TR = 256
B = 64
AHEAD = 4

HIGHEST = lax.Precision.HIGHEST
VMEM = pltpu.VMEM
F32 = jnp.float32
MESH = pl.DeviceIdType.MESH


def hdot(a, b):
    return jnp.dot(a, b, precision=HIGHEST, preferred_element_type=F32)


def hdot_t(a, b):
    return lax.dot_general(a, b, (((1,), (1,)), ((), ())), precision=HIGHEST, preferred_element_type=F32)


def pick_matrix(pivots, group, rows):
    row = group * rows + lax.broadcasted_iota(jnp.int32, (rows, PW), 0)
    return (row == pivots[...]).astype(F32)


def spread_kernel(tc, tr, lr, blocks, slab, pivots, dense, sel, tcs, trs, lrs, held, own_slab, sem):
    cols, rows = own_slab.shape
    count = held.shape[0]
    parts = sem.shape[0] - 4
    size = count // parts
    tables = [pltpu.make_async_copy(a, b, sem.at[i]) for i, (a, b) in enumerate(((tc, tcs), (tr, trs), (lr, lrs)))]
    rest = pltpu.make_async_copy(slab, own_slab, sem.at[3])
    pieces = [
        pltpu.make_async_copy(
            blocks.at[0, pl.ds(i * size, size)], held.at[pl.ds(i * size, size)], sem.at[4 + i]
        )
        for i in range(parts)
    ]
    for copy in tables + pieces + [rest]:
        copy.start()
    dense[...] = jnp.zeros_like(dense)
    pick = pick_matrix(pivots, lax.axis_index("prow"), rows)
    lane = lax.broadcasted_iota(jnp.int32, (NB, TR), 1)
    for copy in tables:
        copy.wait()

    def add(index, carry):
        c = pl.multiple_of(tcs[0, index] * NB, NB)
        r = pl.multiple_of(trs[0, index] * TR, TR)
        block = jnp.where(lane < lrs[0, index], held[index], 0.0)
        dense[pl.ds(c, NB), pl.ds(r, TR)] += block
        return carry

    for i in range(parts):
        pieces[i].wait()
        lax.fori_loop(i * size, (i + 1) * size, add, 0)
    rest.wait()
    own = pl.multiple_of(lax.axis_index("pcol") * cols, cols)
    dense[pl.ds(own, cols), :] += own_slab[...]
    sel[...] = hdot(dense[0:PW, :], pick)


def eliminate(a, every=4):
    groups = B // 8
    eye = (
        lax.broadcasted_iota(jnp.int32, (B, B), 0) == lax.broadcasted_iota(jnp.int32, (B, B), 1)
    ).astype(F32)
    first = jnp.concatenate([a, eye], axis=1)
    second = jnp.concatenate([a.T, eye], axis=1)
    one = [first[8 * g : 8 * g + 8] for g in range(groups)]
    two = [second[8 * g : 8 * g + 8] for g in range(groups)]
    sub = lax.broadcasted_iota(jnp.int32, (8, 2 * B), 0)
    for k in range(B):
        g0, s0 = divmod(k, 8)
        below = sub > s0
        for which, held in enumerate((one, two)):
            col = jnp.broadcast_to(held[g0][:, k : k + 1], (8, 2 * B))
            scaled = jnp.broadcast_to((held[g0] / col)[s0 : s0 + 1, :], (8, 2 * B))
            for g in range(g0 + 1, groups):
                held[g] = held[g] - held[g][:, k : k + 1] * scaled
            fresh = held[g0] - jnp.where(below, col, 0.0) * scaled
            held[g0] = jnp.where(sub == s0, scaled, fresh) if which == 0 else fresh
        if k % every == every - 1:
            yield None
    first = jnp.concatenate(one, axis=0)
    second = jnp.concatenate(two, axis=0)
    return second[:, :B].T, first[:, :B], first[:, B:], second[:, B:].T


def factor(packed, low_inv, up_inv):
    i = lax.broadcasted_iota(jnp.int32, (B, B), 0)
    j = lax.broadcasted_iota(jnp.int32, (B, B), 1)
    for s in range(0, PW, B):
        e = s + B
        low, up, li, ui = yield from eliminate(packed[s:e, s:e])
        li = jnp.where(i >= j, li, 0.0)
        ui = jnp.where(i <= j, ui, 0.0)
        packed[s:e, s:e] = jnp.where(i >= j, low, up)
        low_inv[s:e, :] = li
        up_inv[s:e, :] = ui
        if e < PW:
            right = hdot(li, packed[s:e, e:])
            left = hdot(packed[e:, s:e], ui)
            packed[s:e, e:] = right
            packed[e:, s:e] = left
            packed[e:, e:] = packed[e:, e:] - hdot(left, right)
        yield None


def main_kernel(
    n_row, n_col,
    pivots, dense, sel, out,
    diag_in, diag, panel_in, panel, lead, xr, zl, zr, final, mine, others, moved, pick, packed, low_inv, up_inv,
    x, y,
    diag_sem, panel_sem, lead_sem, x_sem, z_sem, row_sem, moved_sem,
):
    n = n_row * n_col
    cols, rows = out.shape
    group, place = lax.axis_index("prow"), lax.axis_index("pcol")
    me = group * n_col + place
    owners = PW // cols
    per = cols // NB
    reducers, piece = diag.shape[0] // diag_in.shape[1], diag_in.shape[1]
    part = panel_in.shape[1]
    depth = n_col // 2
    level, side = lax.div(place, 2), lax.rem(place, 2)
    steps = depth * per
    half = lax.div(level, depth // 2)

    def device(index):
        return (lax.div(index, n_col), lax.rem(index, n_col))

    def local(ref, sem):
        return pltpu.make_async_copy(ref, ref, sem)

    def send(src, dst, ss, rs, where):
        return pltpu.make_async_remote_copy(
            src_ref=src, dst_ref=dst, send_sem=ss, recv_sem=rs, device_id=where, device_id_type=MESH
        )

    barrier = pltpu.get_barrier_semaphore()

    def greet(d, carry):
        pl.semaphore_signal(barrier, inc=1, device_id=device(lax.rem(me + d, n)), device_id_type=MESH)
        return carry

    lax.fori_loop(1, n, greet, 0)
    pick[...] = pick_matrix(pivots, group, rows)
    pl.semaphore_wait(barrier, n - 1)

    def diag_send(d, carry):
        t = lax.rem(me + d, n)

        def go():
            at = pl.multiple_of(t * piece, piece)
            send(sel.at[pl.ds(at, piece)], diag_in.at[d - 1], diag_sem.at[0], diag_sem.at[1], device(t)).start()

        if reducers == n:
            go()
        else:
            pl.when(t < reducers)(go)
        return carry

    def if_reducer(f):
        if reducers == n:
            f()
        else:
            pl.when(me < reducers)(f)

    def if_not_reducer(f):
        if reducers != n:
            pl.when(me >= reducers)(f)

    lax.fori_loop(1, n, diag_send, 0)

    def x_where(k):
        zone, c = divmod(k, per)
        return half * zone + (1 - half) * (depth - 1 - zone), c

    def x_copy(k):
        goal, c = x_where(k)
        owner = goal * 2 + 1 - side
        at = pl.multiple_of(owner * cols + c * NB, NB)
        copy = send(
            dense.at[pl.ds(at, NB)], xr.at[k], x_sem.at[0, k], x_sem.at[1, k], (group, place + 1 - 2 * side)
        )
        return owner >= owners, copy

    def x_send(k):
        if k < steps:
            live, copy = x_copy(k)
            pl.when(live)(copy.start)

    x_send(0)

    @if_reducer
    def _():
        local(diag_in, diag_sem.at[1]).wait()
        at = pl.multiple_of(me * piece, piece)
        diag[pl.ds(at, piece), :] = sel[pl.ds(at, piece), :] + jnp.sum(diag_in[...], axis=0)

        def diag_spread(d, carry):
            own = diag.at[pl.ds(at, piece)]
            send(own, own, diag_sem.at[2], diag_sem.at[3], device(lax.rem(me + d, n))).start()
            return carry

        lax.fori_loop(1, n, diag_spread, 0)

    def panel_send(d, carry):
        t = lax.rem(place + d, n_col)
        at = pl.multiple_of(t * part, part)
        send(dense.at[pl.ds(at, part)], panel_in.at[d - 1], panel_sem.at[0], panel_sem.at[1], (group, t)).start()
        return carry

    lax.fori_loop(1, n_col, panel_send, 0)
    part_at = pl.multiple_of(place * part, part)

    def panel_reduce():
        local(panel_in, panel_sem.at[1]).wait()
        panel[pl.ds(part_at, part), :] = dense[pl.ds(part_at, part), :] + jnp.sum(panel_in[...], axis=0)

        def panel_spread(d, carry):
            own = panel.at[pl.ds(part_at, part)]
            t = lax.rem(place + d, n_col)
            send(own, own, panel_sem.at[2], panel_sem.at[3], (group, t)).start()
            return carry

        lax.fori_loop(1, n_col, panel_spread, 0)

    def lead_copy(d):
        return send(panel.at[:, 0:PW], lead, lead_sem.at[0, d], lead_sem.at[1, 0], (lax.rem(group + d, n_row), place))

    def panel_finish():
        local(panel.at[pl.ds(0, (n_col - 1) * part)], panel_sem.at[3]).wait()

        @pl.when(group == 0)
        def _():
            for d in range(1, n_row):
                lead_copy(d).start()

    def z_copy(k, way):
        goal, c = x_where(k)
        slot = goal * per + c
        into = zl if way > 0 else zr
        return send(
            xr.at[k], into.at[slot], z_sem.at[0, slot], z_sem.at[1 if way > 0 else 2, slot], (group, place + 2 * way)
        )

    def row_copy(c, d):
        return send(
            mine.at[c], others.at[c, d - 1], row_sem.at[0, c], row_sem.at[1, c], (lax.rem(group + d, n_row), place)
        )

    def moved_copy(c, d):
        return send(
            final.at[c, :, 0:PW], moved.at[c], moved_sem.at[0, c], moved_sem.at[1, c],
            (lax.rem(group + d, n_row), place),
        )

    def chunk(k):
        goal, c = x_where(k)
        owner = goal * 2 + side
        slot = goal * per + c

        @pl.when(owner >= owners)
        def _():
            x_copy(k)[1].wait_recv()
            at = pl.multiple_of(owner * cols + c * NB, NB)
            xr[k] = xr[k] + dense[pl.ds(at, NB), :]

            @pl.when((level <= goal) & (level > 0))
            def _():
                pltpu.make_async_copy(zl.at[slot], zl.at[slot], z_sem.at[1, slot]).wait()
                xr[k] = xr[k] + zl[slot]

            @pl.when((level >= goal) & (level < depth - 1))
            def _():
                pltpu.make_async_copy(zr.at[slot], zr.at[slot], z_sem.at[2, slot]).wait()
                xr[k] = xr[k] + zr[slot]

            @pl.when(level < goal)
            def _():
                z_copy(k, 1).start()

            @pl.when(level > goal)
            def _():
                z_copy(k, -1).start()

            @pl.when(level == goal)
            def _():
                final[c] = xr[k]
                mine[c] = hdot(xr[k], pick[...])
                for d in range(1, n_row):
                    row_copy(c, d).start()

                @pl.when(group == 0)
                def _():
                    for d in range(1, n_row):
                        moved_copy(c, d).start()

    for k in range(1, AHEAD):
        x_send(k)
    chunk(0)
    x_send(AHEAD)
    kept = (reducers - 1) * piece
    local(diag.at[pl.ds(0, kept)], diag_sem.at[3]).wait()
    if_not_reducer(lambda: local(diag.at[pl.ds(0, piece)], diag_sem.at[3]).wait())
    packed[...] = diag[...]
    work = factor(packed, low_inv, up_inv)
    total = (B // 4 + 1) * (PW // B)
    pace = -(-total // (steps - 1))
    for k in range(1, steps):
        chunk(k)
        x_send(k + AHEAD)
        if k == 3:
            panel_reduce()
        if k == 8:
            panel_finish()
        for _ in range(pace):
            next(work, None)
    for _ in work:
        pass

    @pl.when(group > 0)
    def _():
        local(lead, lead_sem.at[1, 0]).wait()

    @pl.when(group == 0)
    def _():
        lead[...] = panel[:, 0:PW]

    head = group == 0
    hit = hdot_t(jnp.ones((8, PW), F32), pick[...])[0:1, :] > 0.5
    x[...] = jnp.where(hit, hdot_t(lead[...], pick[...]), panel[...])
    x[:, 0:PW] = jnp.where(head, diag[...], x[:, 0:PW])
    for s in range(0, PW, B):
        e = s + B
        term = x[s:e, :]
        if s:
            term = term - hdot(packed[s:e, 0:s], x[0:s, :])
        x[s:e, :] = hdot(low_inv[s:e, :], term)

    @pl.when(place >= owners)
    def _():
        for c in range(per):
            local(others.at[c], row_sem.at[1, c]).wait()

            @pl.when(group > 0)
            def _():
                local(moved.at[c], moved_sem.at[1, c]).wait()

            @pl.when(group == 0)
            def _():
                moved[c] = final[c, :, 0:PW]

            mine_all = mine[c] + jnp.sum(others[c], axis=0)
            for s in range(0, PW, B):
                e = s + B
                term = mine_all[:, s:e]
                if s:
                    term = term - hdot(y[:, 0:s], packed[0:s, s:e])
                y[:, s:e] = hdot(term, up_inv[s:e, :])
            swapped = jnp.where(hit, hdot_t(moved[c], pick[...]), final[c])
            lo = c * NB
            out[lo : lo + NB, :] = swapped - hdot(y[...], x[...])
            out[lo : lo + NB, 0:PW] = jnp.where(head, y[...], out[lo : lo + NB, 0:PW])

    @pl.when(place < owners)
    def _():
        x[:, 0:PW] = jnp.where(head, packed[...], x[:, 0:PW])
        off = pl.multiple_of(lax.rem(place, owners) * cols, cols)
        out[...] = x[pl.ds(off, cols), :]

    local(diag.at[pl.ds(0, kept)], diag_sem.at[0]).wait()
    if_not_reducer(lambda: local(diag.at[pl.ds(0, piece)], diag_sem.at[0]).wait())
    if_reducer(lambda: local(diag_in, diag_sem.at[2]).wait())
    local(panel_in, panel_sem.at[0]).wait()
    local(panel_in, panel_sem.at[2]).wait()

    @pl.when(group == 0)
    def _():
        for d in range(1, n_row):
            lead_copy(d).wait_send()

    for k in range(steps):
        live, copy = x_copy(k)
        pl.when(live)(copy.wait_send)
        goal, c = x_where(k)

        @pl.when((goal * 2 + side >= owners) & (level != goal))
        def _():
            z_copy(k, 1).wait_send()

    @pl.when(place >= owners)
    def _():
        for c in range(per):
            local(others.at[c], row_sem.at[0, c]).wait()

            @pl.when(group == 0)
            def _():
                local(others.at[c], moved_sem.at[0, c]).wait()


def shape(*dims):
    return jax.ShapeDtypeStruct(dims, F32)


HBM_SPEC = pl.BlockSpec(memory_space=pltpu.MemorySpace.HBM)
VMEM_SPEC = pl.BlockSpec(memory_space=pltpu.VMEM)
DMA = pltpu.SemaphoreType.DMA


def per_device(
    n_row, n_col, matrix_slab, contributions, target_column, target_rows, live_rows, pivot_index
):
    cols, rows = matrix_slab.shape
    slab_cols = cols * n_col
    count = contributions.shape[1]
    n = n_row * n_col
    parts = 4
    table = pltpu.SMEM((1, count), jnp.int32)
    dense, sel = pl.pallas_call(
        spread_kernel,
        out_shape=(shape(slab_cols, rows), shape(PW, PW)),
        in_specs=[HBM_SPEC] * 5 + [VMEM_SPEC],
        out_specs=(VMEM_SPEC,) * 2,
        scratch_shapes=[table] * 3
        + [VMEM((count, NB, TR), F32), VMEM((cols, rows), F32), DMA((4 + parts,))],
        compiler_params=pltpu.CompilerParams(vmem_limit_bytes=32 * 1024 * 1024),
    )(target_column, target_rows, live_rows, contributions, matrix_slab, pivot_index)
    piece = max(8, PW // n)
    per = cols // NB
    depth = n_col // 2
    steps = depth * per
    part = PW // n_col
    scratch = [
        VMEM((n - 1, piece, PW), F32),
        VMEM((PW, PW), F32),
        VMEM((n_col - 1, part, rows), F32),
        VMEM((PW, rows), F32),
        VMEM((PW, PW), F32),
        VMEM((steps, NB, rows), F32),
        VMEM((steps, NB, rows), F32),
        VMEM((steps, NB, rows), F32),
        VMEM((per, NB, rows), F32),
        VMEM((per, NB, PW), F32),
        VMEM((per, n_row - 1, NB, PW), F32),
        VMEM((per, NB, PW), F32),
        VMEM((rows, PW), F32),
        VMEM((PW, PW), F32),
        VMEM((PW, B), F32),
        VMEM((PW, B), F32),
        VMEM((PW, rows), F32),
        VMEM((NB, PW), F32),
        DMA((4,)),
        DMA((4,)),
        DMA((2, n_row)),
        DMA((2, steps)),
        DMA((3, steps)),
        DMA((2, per)),
        DMA((2, per)),
    ]
    return pl.pallas_call(
        functools.partial(main_kernel, n_row, n_col),
        out_shape=shape(cols, rows),
        in_specs=[VMEM_SPEC] * 3,
        out_specs=VMEM_SPEC,
        scratch_shapes=scratch,
        compiler_params=pltpu.CompilerParams(
            collective_id=0, has_side_effects=True, vmem_limit_bytes=32 * 1024 * 1024
        ),
    )(pivot_index, dense, sel)


def solution(mesh):
    placed = (
        P("pcol", "prow"),
        P("prow", "pcol", None, None),
        P("prow", "pcol"),
        P("prow", "pcol"),
        P("prow", "pcol"),
        P(),
    )
    body = functools.partial(per_device, mesh.shape["prow"], mesh.shape["pcol"])

    def whole(*args):
        return jax.shard_map(
            body, mesh=mesh, in_specs=placed, out_specs=P("pcol", "prow"), check_vma=False
        )(*args)

    return whole
```

```python
import functools

import jax
import jax.numpy as jnp
from jax import lax
from jax.experimental import pallas as pl
from jax.experimental.pallas import tpu as pltpu
from jax.sharding import PartitionSpec as P

PW = 256
NB = 64
TR = 256
B = 64
LAG = 3

HIGHEST = lax.Precision.HIGHEST
VMEM = pltpu.VMEM
F32 = jnp.float32
MESH = pl.DeviceIdType.MESH


def hdot(a, b):
    return jnp.dot(a, b, precision=HIGHEST, preferred_element_type=F32)


def hdot_t(a, b):
    return lax.dot_general(a, b, (((1,), (1,)), ((), ())), precision=HIGHEST, preferred_element_type=F32)


def pick_matrix(pivots, group, rows):
    row = group * rows + lax.broadcasted_iota(jnp.int32, (rows, PW), 0)
    return (row == pivots[...]).astype(F32)


def spread_kernel(tc, tr, lr, blocks, slab, pivots, dense, sel, tcs, trs, lrs, held, own_slab, pivot_row, sem):
    cols, rows = own_slab.shape
    count = held.shape[0]
    parts = sem.shape[0] - 5
    size = count // parts
    tables = [pltpu.make_async_copy(a, b, sem.at[i]) for i, (a, b) in enumerate(((tc, tcs), (tr, trs), (lr, lrs)))]
    rest = pltpu.make_async_copy(slab, own_slab, sem.at[3])
    order = pltpu.make_async_copy(pivots, pivot_row, sem.at[4])
    pieces = [
        pltpu.make_async_copy(
            blocks.at[0, pl.ds(i * size, size)], held.at[pl.ds(i * size, size)], sem.at[5 + i]
        )
        for i in range(parts)
    ]
    for copy in tables + pieces + [rest, order]:
        copy.start()
    dense[...] = jnp.zeros_like(dense)
    lane = lax.broadcasted_iota(jnp.int32, (NB, TR), 1)
    for copy in tables:
        copy.wait()

    def add(index, carry):
        c = pl.multiple_of(tcs[0, index] * NB, NB)
        r = pl.multiple_of(trs[0, index] * TR, TR)
        block = jnp.where(lane < lrs[0, index], held[index], 0.0)
        dense[pl.ds(c, NB), pl.ds(r, TR)] += block
        return carry

    for i in range(parts):
        pieces[i].wait()
        lax.fori_loop(i * size, (i + 1) * size, add, 0)
    rest.wait()
    own = pl.multiple_of(lax.axis_index("pcol") * cols, cols)
    dense[pl.ds(own, cols), :] += own_slab[...]
    order.wait()
    sel[...] = hdot(dense[0:PW, :], pick_matrix(pivot_row, lax.axis_index("prow"), rows))


def eliminate(a, every=4):
    groups = B // 8
    eye = (
        lax.broadcasted_iota(jnp.int32, (B, B), 0) == lax.broadcasted_iota(jnp.int32, (B, B), 1)
    ).astype(F32)
    first = jnp.concatenate([a, eye], axis=1)
    second = jnp.concatenate([a.T, eye], axis=1)
    one = [first[8 * g : 8 * g + 8] for g in range(groups)]
    two = [second[8 * g : 8 * g + 8] for g in range(groups)]
    sub = lax.broadcasted_iota(jnp.int32, (8, 2 * B), 0)
    for k in range(B):
        g0, s0 = divmod(k, 8)
        below = sub > s0
        for which, held in enumerate((one, two)):
            col = jnp.broadcast_to(held[g0][:, k : k + 1], (8, 2 * B))
            scaled = jnp.broadcast_to((held[g0] / col)[s0 : s0 + 1, :], (8, 2 * B))
            for g in range(g0 + 1, groups):
                held[g] = held[g] - held[g][:, k : k + 1] * scaled
            fresh = held[g0] - jnp.where(below, col, 0.0) * scaled
            held[g0] = jnp.where(sub == s0, scaled, fresh) if which == 0 else fresh
        if k % every == every - 1:
            yield None
    first = jnp.concatenate(one, axis=0)
    second = jnp.concatenate(two, axis=0)
    return second[:, :B].T, first[:, :B], first[:, B:], second[:, B:].T


def factor(packed, low_inv, up_inv):
    i = lax.broadcasted_iota(jnp.int32, (B, B), 0)
    j = lax.broadcasted_iota(jnp.int32, (B, B), 1)
    for s in range(0, PW, B):
        e = s + B
        low, up, li, ui = yield from eliminate(packed[s:e, s:e])
        li = jnp.where(i >= j, li, 0.0)
        ui = jnp.where(i <= j, ui, 0.0)
        packed[s:e, s:e] = jnp.where(i >= j, low, up)
        low_inv[s:e, :] = li
        up_inv[s:e, :] = ui
        if e < PW:
            right = hdot(li, packed[s:e, e:])
            left = hdot(packed[e:, s:e], ui)
            packed[s:e, e:] = right
            packed[e:, s:e] = left
            packed[e:, e:] = packed[e:, e:] - hdot(left, right)
        yield None


def main_kernel(
    n_row, n_col,
    pivots, dense, sel, out,
    block_in, block, piece_in, diag, half_in, part_in, panel, lead, xr, zl, zr,
    final, mine, pair_in, others, moved, pick, packed, low_inv, up_inv, x, y,
    pivot_row, pivot_sem, diag_sem, panel_sem, lead_sem, x_sem, z_sem, pair_sem, row_sem, moved_sem,
):
    cols, rows = out.shape
    group, place = lax.axis_index("prow"), lax.axis_index("pcol")
    me = group * n_col + place
    n = n_row * n_col
    owners = PW // cols
    per = cols // NB
    wide = block.shape[0]
    piece = piece_in.shape[1]
    reducers = wide // piece
    pairs = n_row // 2
    depth = n_col // 2
    part = part_in.shape[1]
    steps = depth * per
    level, side = lax.div(place, 2), lax.rem(place, 2)
    row, core = lax.div(group, 2), lax.rem(group, 2)
    near = depth // 2
    half = lax.div(level, near)
    across = (group, place + 1 - 2 * side)
    partner = (group + 1 - 2 * core, place)

    def local(ref, sem):
        return pltpu.make_async_copy(ref, ref, sem)

    def send(src, dst, ss, rs, where):
        return pltpu.make_async_remote_copy(
            src_ref=src, dst_ref=dst, send_sem=ss, recv_sem=rs, device_id=where, device_id_type=MESH
        )

    def rows_of(ref, start, size):
        return ref.at[pl.ds(pl.multiple_of(start, size), size)]

    pivot_copy = pltpu.make_async_copy(pivots, pivot_row, pivot_sem)
    pivot_copy.start()
    barrier = pltpu.get_barrier_semaphore()

    def greet(d, carry):
        t = lax.rem(me + d, n)
        pl.semaphore_signal(
            barrier, inc=1, device_id=(lax.div(t, n_col), lax.rem(t, n_col)), device_id_type=MESH
        )
        return carry

    lax.fori_loop(1, n, greet, 0)
    pivot_copy.wait()
    pick[...] = pick_matrix(pivot_row, group, rows)
    pl.semaphore_wait(barrier, n - 1)

    for d in range(1, n_row):
        t = lax.rem(group + d, n_row)
        send(rows_of(sel, t * wide, wide), block_in.at[d - 1], diag_sem.at[0], diag_sem.at[1], (t, place)).start()
    keep = PW // 2
    half_copy = send(
        rows_of(dense, (1 - side) * keep, keep), half_in, panel_sem.at[0], panel_sem.at[1], across
    )
    half_copy.start()

    def x_where(k):
        zone, c = divmod(k, per)
        if zone < near:
            return half * zone + (1 - half) * (depth - 1 - zone), c
        return half * near + lax.rem(level - half * near + 1 + zone - near, near), c

    def x_copy(k):
        goal, c = x_where(k)
        owner = goal * 2 + 1 - side
        src = rows_of(dense, owner * cols + c * NB, NB)
        return owner >= owners, send(src, xr.at[k], x_sem.at[0, k], x_sem.at[1, k], across)

    def x_send(k):
        if k < steps:
            live, copy = x_copy(k)
            pl.when(live)(copy.start)

    def if_reducer(f):
        if reducers == n_col:
            f()
        else:
            pl.when(place < reducers)(f)

    def if_not_reducer(f):
        if reducers != n_col:
            pl.when(place >= reducers)(f)

    local(block_in, diag_sem.at[1]).wait()
    at = pl.multiple_of(group * wide, wide)
    block[...] = sel[pl.ds(at, wide), :] + jnp.sum(block_in[...], axis=0)

    def piece_send(d, carry):
        t = lax.rem(place + d, n_col)

        def go():
            send(
                rows_of(block, t * piece, piece), piece_in.at[d - 1], diag_sem.at[2], diag_sem.at[3], (group, t)
            ).start()

        if reducers == n_col:
            go()
        else:
            pl.when(t < reducers)(go)
        return carry

    lax.fori_loop(1, n_col, piece_send, 0)
    x_send(0)

    def panel_middle():
        half_copy.wait_recv()
        at = pl.multiple_of(side * keep, keep)
        half_in[...] = half_in[...] + dense[pl.ds(at, keep), :]
        for d in range(1, depth):
            t = lax.rem(level + d, depth)
            send(
                rows_of(half_in, t * part, part), part_in.at[d - 1], panel_sem.at[2], panel_sem.at[3],
                (group, t * 2 + side),
            ).start()

    part_at = pl.multiple_of(side * keep + level * part, part)
    twin_at = pl.multiple_of((1 - side) * keep + level * part, part)

    def panel_sum():
        local(part_in, panel_sem.at[3]).wait()
        mid = pl.multiple_of(level * part, part)
        panel[pl.ds(part_at, part), :] = half_in[pl.ds(mid, part), :] + jnp.sum(part_in[...], axis=0)
        panel_twin(part_at).start()
        panel_spread(part_at, 4)

    def panel_twin(at):
        own = panel.at[pl.ds(at, part)]
        return send(own, own, panel_sem.at[6], panel_sem.at[7], across)

    def panel_spread(at, sem):
        own = panel.at[pl.ds(at, part)]
        for d in range(1, depth):
            t = lax.rem(level + d, depth)
            send(own, own, panel_sem.at[sem], panel_sem.at[sem + 1], (group, t * 2 + side)).start()

    def panel_gather():
        panel_twin(twin_at).wait_recv()
        panel_spread(twin_at, 8)

    def lead_copy(d):
        return send(
            panel.at[:, 0:PW], lead, lead_sem.at[0, d], lead_sem.at[1, 0], (lax.rem(group + d, n_row), place)
        )

    def panel_finish():
        local(part_in, panel_sem.at[5]).wait()
        local(part_in, panel_sem.at[9]).wait()

        @pl.when(group == 0)
        def _():
            for d in range(1, n_row):
                lead_copy(d).start()

    panel_middle()
    diag_at = pl.multiple_of(group * wide + place * piece, piece)

    @if_reducer
    def _():
        local(piece_in, diag_sem.at[3]).wait()
        mid = pl.multiple_of(place * piece, piece)
        diag[pl.ds(diag_at, piece), :] = block[pl.ds(mid, piece), :] + jnp.sum(piece_in[...], axis=0)

        def piece_spread(d, carry):
            own = diag.at[pl.ds(diag_at, piece)]
            send(own, own, diag_sem.at[4], diag_sem.at[5], (group, lax.rem(place + d, n_col))).start()
            return carry

        lax.fori_loop(1, n_col, piece_spread, 0)

    x_send(1)
    x_send(2)

    def z_copy(k, way):
        goal, c = x_where(k)
        slot = goal * per + c
        into = zl if way > 0 else zr
        return send(
            xr.at[k], into.at[slot], z_sem.at[0, slot], z_sem.at[1 if way > 0 else 2, slot], (group, place + 2 * way)
        )

    def pair_copy(c):
        return send(mine.at[pl.ds(c * NB, NB)], pair_in.at[pl.ds(c * NB, NB)], pair_sem.at[0, c], pair_sem.at[1, c], partner)

    def moved_pair(c):
        return send(
            final.at[pl.ds(c * NB, NB), 0:PW], moved.at[pl.ds(c * NB, NB)], moved_sem.at[0, c], moved_sem.at[1, c],
            partner,
        )

    def row_copy(c, d):
        where = (lax.rem(row + d, pairs) * 2 + core, place)
        return send(
            pair_in.at[pl.ds(c * NB, NB)], others.at[c, d - 1], row_sem.at[0, c], row_sem.at[1, c], where
        )

    def moved_copy(c, d):
        where = (lax.rem(row + d, pairs) * 2 + core, place)
        into = moved.at[pl.ds(c * NB, NB)]
        return send(into, into, moved_sem.at[2, c], moved_sem.at[1, c], where)

    def goal_of(k):
        goal, c = x_where(k)
        return goal, c, goal * 2 + side, goal * per + c

    def x_part(k):
        goal, c, owner, slot = goal_of(k)

        @pl.when(owner >= owners)
        def _():
            x_copy(k)[1].wait_recv()
            at = pl.multiple_of(owner * cols + c * NB, NB)
            xr[k] = xr[k] + dense[pl.ds(at, NB), :]

            @pl.when((level < goal) & (level == 0))
            def _():
                z_copy(k, 1).start()

            @pl.when((level > goal) & (level == depth - 1))
            def _():
                z_copy(k, -1).start()

    def z_part(k):
        goal, c, owner, slot = goal_of(k)

        @pl.when(owner >= owners)
        def _():
            @pl.when((level <= goal) & (level > 0))
            def _():
                pltpu.make_async_copy(zl.at[slot], zl.at[slot], z_sem.at[1, slot]).wait()
                xr[k] = xr[k] + zl[slot]

            @pl.when((level >= goal) & (level < depth - 1))
            def _():
                pltpu.make_async_copy(zr.at[slot], zr.at[slot], z_sem.at[2, slot]).wait()
                xr[k] = xr[k] + zr[slot]

            @pl.when((level < goal) & (level > 0))
            def _():
                z_copy(k, 1).start()

            @pl.when((level > goal) & (level < depth - 1))
            def _():
                z_copy(k, -1).start()

            if k >= steps - per:
                final[c * NB : c * NB + NB, :] = xr[k]
                mine[c * NB : c * NB + NB, :] = hdot(xr[k], pick[...])
                pair_copy(c).start()
                pl.when(group == 0)(moved_pair(c).start)

    def row_part(c):
        @pl.when(place >= owners)
        def _():
            lo = c * NB
            pair_copy(c).wait()
            pair_in[lo : lo + NB, :] = pair_in[lo : lo + NB, :] + mine[lo : lo + NB, :]
            for d in range(1, pairs):
                row_copy(c, d).start()

            @pl.when(group == 0)
            def _():
                moved[lo : lo + NB, :] = final[lo : lo + NB, 0:PW]

            @pl.when(group == 1)
            def _():
                local(moved.at[pl.ds(lo, NB)], moved_sem.at[1, c]).wait()

            @pl.when(row == 0)
            def _():
                for d in range(1, pairs):
                    moved_copy(c, d).start()

    x_part(0)
    kept = (reducers - 1) * piece
    local(diag.at[pl.ds(0, kept)], diag_sem.at[5]).wait()
    if_not_reducer(lambda: local(diag.at[pl.ds(0, piece)], diag_sem.at[5]).wait())
    for d in range(1, n_row):
        own = rows_of(diag, group * wide, wide)
        send(own, own, diag_sem.at[6], diag_sem.at[7], (lax.rem(group + d, n_row), place)).start()
    x_send(3)
    x_send(4)
    panel_sum()
    x_part(1)
    x_part(2)
    local(diag.at[pl.ds(0, (n_row - 1) * wide)], diag_sem.at[7]).wait()
    packed[...] = diag[...]
    x_send(5)
    work = factor(packed, low_inv, up_inv)
    head = group == 0
    hit = hdot_t(jnp.ones((8, PW), F32), pick[...])[0:1, :] > 0.5

    def solve_x():
        @pl.when(group > 0)
        def _():
            local(lead, lead_sem.at[1, 0]).wait()

        @pl.when(group == 0)
        def _():
            lead[...] = panel[:, 0:PW]

        x[...] = jnp.where(hit, hdot_t(lead[...], pick[...]), panel[...])
        x[:, 0:PW] = jnp.where(head, diag[...], x[:, 0:PW])
        for s in range(0, PW, B):
            e = s + B
            term = x[s:e, :]
            if s:
                term = term - hdot(packed[s:e, 0:s], x[0:s, :])
            x[s:e, :] = hdot(low_inv[s:e, :], term)

    def finish(begin, end):
        @pl.when(place >= owners)
        def _():
            for c in range(begin, end):
                lo = c * NB
                local(others.at[c], row_sem.at[1, c]).wait()

                @pl.when(row > 0)
                def _():
                    local(moved.at[pl.ds(lo, NB)], moved_sem.at[1, c]).wait()

                mine[lo : lo + NB, :] = pair_in[lo : lo + NB, :] + jnp.sum(others[c], axis=0)
            lo, hi = begin * NB, end * NB
            for s in range(0, PW, B):
                e = s + B
                term = mine[lo:hi, s:e]
                if s:
                    term = term - hdot(y[lo:hi, 0:s], packed[0:s, s:e])
                y[lo:hi, s:e] = hdot(term, up_inv[s:e, :])
            swapped = jnp.where(hit, hdot_t(moved[lo:hi, :], pick[...]), final[lo:hi, :])
            out[lo:hi, :] = swapped - hdot(y[lo:hi, :], x[...])
            out[lo:hi, 0:PW] = jnp.where(head, y[lo:hi, :], out[lo:hi, 0:PW])

    first = 3
    far = near * per
    total = (B // 4 + 1) * (PW // B)
    pace = -(-total // (steps - first - per))
    for k in range(first, steps):
        x_part(k)
        if k - LAG < far:
            z_part(k - LAG)
        if k >= far:
            z_part(k)
        x_send(k + LAG)
        if k > steps - per:
            row_part(k - steps + per - 1)
        if k == 5:
            panel_gather()
        if k == 8:
            panel_finish()
        for _ in range(pace):
            next(work, None)
        if k == steps - 2:
            for _ in work:
                pass
            solve_x()
    row_part(per - 1)
    if per > 1:
        finish(0, per - 1)
    finish(per - 1, per)

    @pl.when(place < owners)
    def _():
        x[:, 0:PW] = jnp.where(head, packed[...], x[:, 0:PW])
        off = pl.multiple_of(lax.rem(place, owners) * cols, cols)
        out[...] = x[pl.ds(off, cols), :]

    local(block_in, diag_sem.at[0]).wait()
    local(block.at[pl.ds(0, kept)], diag_sem.at[2]).wait()
    if_not_reducer(lambda: local(block.at[pl.ds(0, piece)], diag_sem.at[2]).wait())
    if_reducer(lambda: local(piece_in, diag_sem.at[4]).wait())
    local(block_in, diag_sem.at[6]).wait()
    half_copy.wait_send()
    local(part_in, panel_sem.at[2]).wait()
    local(part_in, panel_sem.at[4]).wait()
    panel_twin(part_at).wait_send()
    local(part_in, panel_sem.at[8]).wait()

    @pl.when(group == 0)
    def _():
        for d in range(1, n_row):
            lead_copy(d).wait_send()

    for k in range(steps):
        live, copy = x_copy(k)
        pl.when(live)(copy.wait_send)
        goal, c, owner, slot = goal_of(k)

        @pl.when((owner >= owners) & (level != goal))
        def _():
            z_copy(k, 1).wait_send()

    @pl.when(place >= owners)
    def _():
        for c in range(per):
            local(others.at[c], row_sem.at[0, c]).wait()
            pl.when(group == 0)(moved_pair(c).wait_send)

            @pl.when(row == 0)
            def _():
                local(others.at[c], moved_sem.at[2, c]).wait()


def stay(array):
    return pltpu.with_memory_space_constraint(array, pltpu.MemorySpace.HBM)


def shape(*dims):
    return jax.ShapeDtypeStruct(dims, F32)


HBM_SPEC = pl.BlockSpec(memory_space=pltpu.MemorySpace.HBM)
VMEM_SPEC = pl.BlockSpec(memory_space=pltpu.VMEM)
DMA = pltpu.SemaphoreType.DMA


def per_device(
    n_row, n_col, matrix_slab, contributions, target_column, target_rows, live_rows, pivot_index
):
    cols, rows = matrix_slab.shape
    slab_cols = cols * n_col
    count = contributions.shape[1]
    parts = 4
    table = pltpu.SMEM((1, count), jnp.int32)
    dense, sel = pl.pallas_call(
        spread_kernel,
        out_shape=(shape(slab_cols, rows), shape(PW, PW)),
        in_specs=[HBM_SPEC] * 6,
        out_specs=(VMEM_SPEC,) * 2,
        scratch_shapes=[table] * 3
        + [
            VMEM((count, NB, TR), F32),
            VMEM((cols, rows), F32),
            VMEM((1, PW), jnp.int32),
            DMA((5 + parts,)),
        ],
        compiler_params=pltpu.CompilerParams(vmem_limit_bytes=32 * 1024 * 1024),
    )(*map(stay, (target_column, target_rows, live_rows, contributions, matrix_slab, pivot_index)))
    wide = PW // n_row
    piece = max(8, wide // n_col)
    per = cols // NB
    depth = n_col // 2
    steps = depth * per
    part = PW // n_col
    scratch = [
        VMEM((n_row - 1, wide, PW), F32),
        VMEM((wide, PW), F32),
        VMEM((n_col - 1, piece, PW), F32),
        VMEM((PW, PW), F32),
        VMEM((PW // 2, rows), F32),
        VMEM((depth - 1, part, rows), F32),
        VMEM((PW, rows), F32),
        VMEM((PW, PW), F32),
        VMEM((steps, NB, rows), F32),
        VMEM((steps, NB, rows), F32),
        VMEM((steps, NB, rows), F32),
        VMEM((cols, rows), F32),
        VMEM((cols, PW), F32),
        VMEM((cols, PW), F32),
        VMEM((per, n_row // 2 - 1, NB, PW), F32),
        VMEM((cols, PW), F32),
        VMEM((rows, PW), F32),
        VMEM((PW, PW), F32),
        VMEM((PW, B), F32),
        VMEM((PW, B), F32),
        VMEM((PW, rows), F32),
        VMEM((cols, PW), F32),
        VMEM((1, PW), jnp.int32),
        DMA,
        DMA((8,)),
        DMA((10,)),
        DMA((2, n_row)),
        DMA((2, steps)),
        DMA((3, steps)),
        DMA((2, per)),
        DMA((2, per)),
        DMA((3, per)),
    ]
    return pl.pallas_call(
        functools.partial(main_kernel, n_row, n_col),
        out_shape=shape(cols, rows),
        in_specs=[HBM_SPEC] + [VMEM_SPEC] * 2,
        out_specs=VMEM_SPEC,
        scratch_shapes=scratch,
        compiler_params=pltpu.CompilerParams(
            collective_id=0, has_side_effects=True, vmem_limit_bytes=32 * 1024 * 1024
        ),
    )(stay(pivot_index), dense, sel)


def solution(mesh):
    placed = (
        P("pcol", "prow"),
        P("prow", "pcol", None, None),
        P("prow", "pcol"),
        P("prow", "pcol"),
        P("prow", "pcol"),
        P(),
    )
    body = functools.partial(per_device, mesh.shape["prow"], mesh.shape["pcol"])

    def whole(*args):
        return jax.shard_map(
            body, mesh=mesh, in_specs=placed, out_specs=P("pcol", "prow"), check_vma=False
        )(*args)

    return whole
```

```python
import functools

import jax
import jax.numpy as jnp
from jax import lax
from jax.experimental import pallas as pl
from jax.experimental.pallas import tpu as pltpu
from jax.sharding import PartitionSpec as P

PW = 256
NB = 64
TR = 256
B = 64
LAG = 2
AHEAD = 4
PACE = 8

HIGHEST = lax.Precision.HIGHEST
VMEM = pltpu.VMEM
F32 = jnp.float32
MESH = pl.DeviceIdType.MESH


def hdot(a, b):
    return jnp.dot(a, b, precision=HIGHEST, preferred_element_type=F32)


def hdot_t(a, b):
    return lax.dot_general(a, b, (((1,), (1,)), ((), ())), precision=HIGHEST, preferred_element_type=F32)


def pick_matrix(pivots, group, rows):
    row = group * rows + lax.broadcasted_iota(jnp.int32, (rows, PW), 0)
    return (row == pivots[...]).astype(F32)


def spread_kernel(tc, tr, lr, blocks, slab, pivots, dense, sel, tcs, trs, lrs, held, own_slab, pivot_row, sem):
    cols, rows = own_slab.shape
    count = held.shape[0]
    parts = sem.shape[0] - 5
    size = count // parts
    tables = [pltpu.make_async_copy(a, b, sem.at[i]) for i, (a, b) in enumerate(((tc, tcs), (tr, trs), (lr, lrs)))]
    rest = pltpu.make_async_copy(slab, own_slab, sem.at[3])
    order = pltpu.make_async_copy(pivots, pivot_row, sem.at[4])
    pieces = [
        pltpu.make_async_copy(
            blocks.at[0, pl.ds(i * size, size)], held.at[pl.ds(i * size, size)], sem.at[5 + i]
        )
        for i in range(parts)
    ]
    for copy in tables + pieces + [rest, order]:
        copy.start()
    dense[...] = jnp.zeros_like(dense)
    lane = lax.broadcasted_iota(jnp.int32, (NB, TR), 1)
    for copy in tables:
        copy.wait()

    def add(index, carry):
        c = pl.multiple_of(tcs[0, index] * NB, NB)
        r = pl.multiple_of(trs[0, index] * TR, TR)
        block = jnp.where(lane < lrs[0, index], held[index], 0.0)
        dense[pl.ds(c, NB), pl.ds(r, TR)] += block
        return carry

    for i in range(parts):
        pieces[i].wait()
        lax.fori_loop(i * size, (i + 1) * size, add, 0)
    rest.wait()
    own = pl.multiple_of(lax.axis_index("pcol") * cols, cols)
    dense[pl.ds(own, cols), :] += own_slab[...]
    order.wait()
    sel[...] = hdot(dense[0:PW, :], pick_matrix(pivot_row, lax.axis_index("prow"), rows))


def eliminate(a, every=4):
    groups = B // 8
    eye = (
        lax.broadcasted_iota(jnp.int32, (B, B), 0) == lax.broadcasted_iota(jnp.int32, (B, B), 1)
    ).astype(F32)
    first = jnp.concatenate([a, eye], axis=1)
    second = jnp.concatenate([a.T, eye], axis=1)
    one = [first[8 * g : 8 * g + 8] for g in range(groups)]
    two = [second[8 * g : 8 * g + 8] for g in range(groups)]
    sub = lax.broadcasted_iota(jnp.int32, (8, 2 * B), 0)
    for k in range(B):
        g0, s0 = divmod(k, 8)
        below = sub > s0
        for which, held in enumerate((one, two)):
            col = jnp.broadcast_to(held[g0][:, k : k + 1], (8, 2 * B))
            scaled = jnp.broadcast_to((held[g0] / col)[s0 : s0 + 1, :], (8, 2 * B))
            for g in range(g0 + 1, groups):
                held[g] = held[g] - held[g][:, k : k + 1] * scaled
            fresh = held[g0] - jnp.where(below, col, 0.0) * scaled
            held[g0] = jnp.where(sub == s0, scaled, fresh) if which == 0 else fresh
        if k % every == every - 1:
            yield None
    first = jnp.concatenate(one, axis=0)
    second = jnp.concatenate(two, axis=0)
    return second[:, :B].T, first[:, :B], first[:, B:], second[:, B:].T


def factor(packed, low_inv, up_inv):
    i = lax.broadcasted_iota(jnp.int32, (B, B), 0)
    j = lax.broadcasted_iota(jnp.int32, (B, B), 1)
    for s in range(0, PW, B):
        e = s + B
        low, up, li, ui = yield from eliminate(packed[s:e, s:e])
        li = jnp.where(i >= j, li, 0.0)
        ui = jnp.where(i <= j, ui, 0.0)
        packed[s:e, s:e] = jnp.where(i >= j, low, up)
        low_inv[s:e, :] = li
        up_inv[s:e, :] = ui
        if e < PW:
            right = hdot(li, packed[s:e, e:])
            left = hdot(packed[e:, s:e], ui)
            packed[s:e, e:] = right
            packed[e:, s:e] = left
            packed[e:, e:] = packed[e:, e:] - hdot(left, right)
        yield None


def main_kernel(
    n_row, n_col,
    pivots, dense, sel, out,
    block_in, block, piece_in, diag, level_in, level_sum, twin_in, band_sum, lead, xr, zl, zr,
    final, mine, pair_in, others, moved, pick, packed, low_inv, up_inv, x, y, inverse,
    pivot_row, pivot_sem, diag_sem, panel_sem, lead_sem, chain_sem, x_sem, z_sem, pair_sem, row_sem, moved_sem,
):
    cols, rows = out.shape
    group, place = lax.axis_index("prow"), lax.axis_index("pcol")
    me = group * n_col + place
    n = n_row * n_col
    owners = PW // cols
    per = cols // NB
    wide = block.shape[0]
    piece = piece_in.shape[1]
    reducers = wide // piece
    pairs = n_row // 2
    depth = n_col // 2
    band = twin_in.shape[0]
    steps = depth * per
    level, side = lax.div(place, 2), lax.rem(place, 2)
    row, core = lax.div(group, 2), lax.rem(group, 2)
    near = depth // 2
    half = lax.div(level, near)
    across = (group, place + 1 - 2 * side)
    partner = (group + 1 - 2 * core, place)

    def local(ref, sem):
        return pltpu.make_async_copy(ref, ref, sem)

    def send(src, dst, ss, rs, where):
        return pltpu.make_async_remote_copy(
            src_ref=src, dst_ref=dst, send_sem=ss, recv_sem=rs, device_id=where, device_id_type=MESH
        )

    def rows_of(ref, start, size):
        return ref.at[pl.ds(pl.multiple_of(start, size), size)]

    pivot_copy = pltpu.make_async_copy(pivots, pivot_row, pivot_sem)
    pivot_copy.start()
    barrier = pltpu.get_barrier_semaphore()

    def greet(d, carry):
        t = lax.rem(me + d, n)
        pl.semaphore_signal(
            barrier, inc=1, device_id=(lax.div(t, n_col), lax.rem(t, n_col)), device_id_type=MESH
        )
        return carry

    lax.fori_loop(1, n, greet, 0)
    pivot_copy.wait()
    pick[...] = pick_matrix(pivot_row, group, rows)
    head = group == 0
    hit = hdot_t(jnp.ones((8, PW), F32), pick[...])[0:1, :] > 0.5
    pl.semaphore_wait(barrier, n - 1)

    for d in range(1, n_row):
        t = lax.rem(group + d, n_row)
        send(rows_of(sel, t * wide, wide), block_in.at[d - 1], diag_sem.at[0], diag_sem.at[1], (t, place)).start()
    def level_send(d):
        t = lax.rem(level + d, depth)
        send(
            rows_of(dense, t * band, band), level_in.at[d - 1], panel_sem.at[0], panel_sem.at[1],
            (group, t * 2 + side),
        ).start()

    def x_where(k):
        zone, c = divmod(k, per)

        def far_goal(i):
            return half * i + (1 - half) * (depth - 1 - i)

        def near_goal(i):
            return half * near + lax.rem(level - half * near + 1 + i, near)

        goal = far_goal(zone) if zone < near else near_goal(zone - near)
        if near == 2 and zone in (1, 2):
            edge = 1 - lax.rem(lax.div(level + 1, 2), 2)
            goal = edge * goal + (1 - edge) * (near_goal(0) if zone == 1 else far_goal(1))
        return goal, c

    def x_copy(k):
        goal, c = x_where(k)
        owner = goal * 2 + 1 - side
        src = rows_of(dense, owner * cols + c * NB, NB)
        return owner >= owners, send(src, xr.at[k], x_sem.at[0, k], x_sem.at[1, k], across)

    def x_send(k):
        if k < steps:
            live, copy = x_copy(k)
            pl.when(live)(copy.start)

    def if_reducer(f):
        if reducers == n_col:
            f()
        else:
            pl.when(place < reducers)(f)

    def if_not_reducer(f):
        if reducers != n_col:
            pl.when(place >= reducers)(f)

    level_send(1)
    x_send(0)
    local(block_in, diag_sem.at[1]).wait()
    at = pl.multiple_of(group * wide, wide)
    block[...] = sel[pl.ds(at, wide), :] + jnp.sum(block_in[...], axis=0)

    def piece_send(d, carry):
        t = lax.rem(place + d, n_col)

        def go():
            send(
                rows_of(block, t * piece, piece), piece_in.at[d - 1], diag_sem.at[2], diag_sem.at[3], (group, t)
            ).start()

        if reducers == n_col:
            go()
        else:
            pl.when(t < reducers)(go)
        return carry

    lax.fori_loop(1, n_col, piece_send, 0)
    level_send(depth - 1)
    x_send(1)
    own_band = pl.multiple_of(level * band, band)

    def twin_copy():
        return send(level_sum, twin_in, panel_sem.at[2], panel_sem.at[3], across)

    def panel_sum():
        local(level_in, panel_sem.at[1]).wait()
        level_sum[...] = dense[pl.ds(own_band, band), :] + jnp.sum(level_in[...], axis=0)
        twin_copy().start()

    def lead_copy(d):
        return send(
            band_sum.at[:, 0:PW], lead, lead_sem.at[0, d], lead_sem.at[1, 0], (lax.rem(group + d, n_row), place)
        )

    def panel_twin():
        twin_copy().wait_recv()
        band_sum[...] = level_sum[...] + twin_in[...]

        @pl.when(group == 0)
        def _():
            for d in range(1, n_row):
                lead_copy(d).start()

    def chain_copy(index, way):
        own = rows_of(x, index * band, band)
        return send(
            own, own, chain_sem.at[0 if way > 0 else 1, index], chain_sem.at[2, index], (group, place + 2 * way)
        )

    def panel_swap():
        @pl.when(group > 0)
        def _():
            local(lead, lead_sem.at[1, 0]).wait()

        @pl.when(group == 0)
        def _():
            lead[...] = band_sum[:, 0:PW]

        x[pl.ds(own_band, band), :] = jnp.where(hit, hdot_t(lead[...], pick[...]), band_sum[...])
        pl.when(level < depth - 1)(chain_copy(level, 1).start)
        pl.when(level > 0)(chain_copy(level, -1).start)

    def panel_step(s, way, final_stop):
        index = level - s * way
        inside = (index >= 0) & (index < depth)
        index = lax.rem(index + depth, depth)
        end = (level == depth - 1) if way > 0 else (level == 0)

        @pl.when(inside & (end if final_stop else jnp.logical_not(end)))
        def _():
            chain_copy(index, way).wait_recv()
            if not final_stop:
                chain_copy(index, way).start()

    def panel_stage(s):
        for way in (1, -1):
            panel_step(s, way, False)

    def panel_collect():
        for s in range(1, depth):
            for way in (1, -1):
                panel_step(s, way, True)

    def panel_sent():
        for b in range(depth):
            pl.when((b <= level) & (level < depth - 1))(chain_copy(b, 1).wait_send)
            pl.when((b >= level) & (level > 0))(chain_copy(b, -1).wait_send)

    diag_at = pl.multiple_of(group * wide + place * piece, piece)

    @if_reducer
    def _():
        local(piece_in, diag_sem.at[3]).wait()
        mid = pl.multiple_of(place * piece, piece)
        diag[pl.ds(diag_at, piece), :] = block[pl.ds(mid, piece), :] + jnp.sum(piece_in[...], axis=0)

        def piece_spread(d, carry):
            own = diag.at[pl.ds(diag_at, piece)]
            send(own, own, diag_sem.at[4], diag_sem.at[5], (group, lax.rem(place + d, n_col))).start()
            return carry

        lax.fori_loop(1, n_col, piece_spread, 0)

    for d in range(2, depth - 1):
        level_send(d)
    x_send(2)

    def z_copy(k, way):
        goal, c = x_where(k)
        slot = goal * per + c
        into = zl if way > 0 else zr
        return send(
            xr.at[k], into.at[slot], z_sem.at[0, slot], z_sem.at[1 if way > 0 else 2, slot], (group, place + 2 * way)
        )

    def pair_copy(c):
        return send(mine.at[pl.ds(c * NB, NB)], pair_in.at[pl.ds(c * NB, NB)], pair_sem.at[0, c], pair_sem.at[1, c], partner)

    def moved_pair(c):
        return send(
            final.at[pl.ds(c * NB, NB), 0:PW], moved.at[pl.ds(c * NB, NB)], moved_sem.at[0, c], moved_sem.at[1, c],
            partner,
        )

    def moved_pass(c):
        into = moved.at[pl.ds(c * NB, NB)]
        return send(into, into, moved_sem.at[0, c], moved_sem.at[1, c], partner)

    def row_copy(c, d):
        where = (lax.rem(row + d, pairs) * 2 + core, place)
        return send(
            pair_in.at[pl.ds(c * NB, NB)], others.at[c, d - 1], row_sem.at[0, c], row_sem.at[1, c], where
        )

    def moved_copy(c, d):
        where = (lax.rem(row + d, pairs) * 2 + core, place)
        into = moved.at[pl.ds(c * NB, NB)]
        return send(into, into, moved_sem.at[2, c], moved_sem.at[1, c], where)

    def goal_of(k):
        goal, c = x_where(k)
        return goal, c, goal * 2 + side, goal * per + c

    def x_part(k):
        goal, c, owner, slot = goal_of(k)

        @pl.when(owner >= owners)
        def _():
            x_copy(k)[1].wait_recv()
            at = pl.multiple_of(owner * cols + c * NB, NB)
            xr[k] = xr[k] + dense[pl.ds(at, NB), :]

            @pl.when((level < goal) & (level == 0))
            def _():
                z_copy(k, 1).start()

            @pl.when((level > goal) & (level == depth - 1))
            def _():
                z_copy(k, -1).start()

    def z_part(k):
        goal, c, owner, slot = goal_of(k)

        @pl.when(owner >= owners)
        def _():
            @pl.when((level <= goal) & (level > 0))
            def _():
                pltpu.make_async_copy(zl.at[slot], zl.at[slot], z_sem.at[1, slot]).wait()
                xr[k] = xr[k] + zl[slot]

            @pl.when((level >= goal) & (level < depth - 1))
            def _():
                pltpu.make_async_copy(zr.at[slot], zr.at[slot], z_sem.at[2, slot]).wait()
                xr[k] = xr[k] + zr[slot]

            @pl.when((level < goal) & (level > 0))
            def _():
                z_copy(k, 1).start()

            @pl.when((level > goal) & (level < depth - 1))
            def _():
                z_copy(k, -1).start()

            if k >= steps - per:
                final[c * NB : c * NB + NB, :] = xr[k]
                mine[c * NB : c * NB + NB, :] = hdot(xr[k], pick[...])
                pair_copy(c).start()
                pl.when(group == 0)(moved_pair(c).start)

    def row_part(c):
        @pl.when(place >= owners)
        def _():
            lo = c * NB
            pair_copy(c).wait()
            pair_in[lo : lo + NB, :] = pair_in[lo : lo + NB, :] + mine[lo : lo + NB, :]
            for d in range(1, pairs):
                row_copy(c, d).start()

            @pl.when(group == 0)
            def _():
                moved[lo : lo + NB, :] = final[lo : lo + NB, 0:PW]

            @pl.when(group == 1)
            def _():
                local(moved.at[pl.ds(lo, NB)], moved_sem.at[1, c]).wait()

            @pl.when(group == 0)
            def _():
                for d in range(1, pairs):
                    moved_copy(c, d).start()

    kept = (reducers - 1) * piece
    local(diag.at[pl.ds(0, kept)], diag_sem.at[5]).wait()
    if_not_reducer(lambda: local(diag.at[pl.ds(0, piece)], diag_sem.at[5]).wait())
    for d in range(1, n_row):
        own = rows_of(diag, group * wide, wide)
        send(own, own, diag_sem.at[6], diag_sem.at[7], (lax.rem(group + d, n_row), place)).start()
    for k in range(3, AHEAD + 1):
        x_send(k)
    x_part(0)
    local(diag.at[pl.ds(0, (n_row - 1) * wide)], diag_sem.at[7]).wait()
    packed[...] = diag[...]

    def all_work():
        yield from factor(packed, low_inv, up_inv)
        inverse[...] = jnp.zeros_like(inverse)
        for s in range(0, PW, B):
            e = s + B
            inverse[s:e, s:e] = up_inv[s:e, :]
            if s:
                term = hdot(packed[0:s, s:e], up_inv[s:e, :])
                inverse[0:s, s:e] = -hdot(inverse[0:s, 0:s], term)
            yield None

    work = all_work()

    def solve_x():
        panel_collect()
        panel_sent()
        x[:, 0:PW] = jnp.where(head, diag[...], x[:, 0:PW])
        for s in range(0, PW, B):
            e = s + B
            term = x[s:e, :]
            if s:
                term = term - hdot(packed[s:e, 0:s], x[0:s, :])
            x[s:e, :] = hdot(low_inv[s:e, :], term)

    def finish(begin, end):
        @pl.when(place >= owners)
        def _():
            for c in range(begin, end):
                lo = c * NB
                local(others.at[c], row_sem.at[1, c]).wait()

                @pl.when(row > 0)
                def _():
                    local(moved.at[pl.ds(lo, NB)], moved_sem.at[1, c]).wait()
                    pl.when(core == 0)(moved_pass(c).start)

                mine[lo : lo + NB, :] = pair_in[lo : lo + NB, :] + jnp.sum(others[c], axis=0)
            lo, hi = begin * NB, end * NB
            y[lo:hi, :] = hdot(mine[lo:hi, :], inverse[...])
            swapped = jnp.where(hit, hdot_t(moved[lo:hi, :], pick[...]), final[lo:hi, :])
            out[lo:hi, :] = swapped - hdot(y[lo:hi, :], x[...])
            out[lo:hi, 0:PW] = jnp.where(head, y[lo:hi, :], out[lo:hi, 0:PW])

    far = near * per
    last = steps - per
    for k in range(1, steps):
        for s in range(1, depth - 1):
            if k == (4 + 2 * s if near == 2 else 5):
                panel_stage(s)
        x_part(k)
        if 0 <= k - LAG < far:
            z_part(k - LAG)
        if k >= far:
            z_part(k)
        if k == 1:
            panel_sum()
            for later in range(AHEAD + 1, steps):
                x_send(later)
        if k == 3:
            panel_twin()
        if k == 4:
            panel_swap()
        for _ in range(PACE):
            next(work, None)
        if k == min(last + 1, steps - 1):
            for _ in work:
                pass
            solve_x()
        if k > last:
            row_part(k - last - 1)
        if k > last + 2:
            finish(k - last - 3, k - last - 2)
    row_part(per - 1)
    for c in range(max(per - 3, 0), per):
        finish(c, c + 1)

    @pl.when(place < owners)
    def _():
        x[:, 0:PW] = jnp.where(head, packed[...], x[:, 0:PW])
        off = pl.multiple_of(lax.rem(place, owners) * cols, cols)
        out[...] = x[pl.ds(off, cols), :]

    local(block_in, diag_sem.at[0]).wait()
    local(block.at[pl.ds(0, kept)], diag_sem.at[2]).wait()
    if_not_reducer(lambda: local(block.at[pl.ds(0, piece)], diag_sem.at[2]).wait())
    if_reducer(lambda: local(piece_in, diag_sem.at[4]).wait())
    local(block_in, diag_sem.at[6]).wait()
    local(level_in, panel_sem.at[0]).wait()
    twin_copy().wait_send()

    @pl.when(group == 0)
    def _():
        for d in range(1, n_row):
            lead_copy(d).wait_send()

    for k in range(steps):
        live, copy = x_copy(k)
        pl.when(live)(copy.wait_send)
        goal, c, owner, slot = goal_of(k)

        @pl.when((owner >= owners) & (level != goal))
        def _():
            z_copy(k, 1).wait_send()

    @pl.when(place >= owners)
    def _():
        for c in range(per):
            local(others.at[c], row_sem.at[0, c]).wait()
            pl.when(core == 0)(moved_pair(c).wait_send)

            @pl.when(group == 0)
            def _():
                local(others.at[c], moved_sem.at[2, c]).wait()


def stay(array):
    return pltpu.with_memory_space_constraint(array, pltpu.MemorySpace.HBM)


def shape(*dims):
    return jax.ShapeDtypeStruct(dims, F32)


HBM_SPEC = pl.BlockSpec(memory_space=pltpu.MemorySpace.HBM)
VMEM_SPEC = pl.BlockSpec(memory_space=pltpu.VMEM)
DMA = pltpu.SemaphoreType.DMA


def per_device(
    n_row, n_col, matrix_slab, contributions, target_column, target_rows, live_rows, pivot_index
):
    cols, rows = matrix_slab.shape
    slab_cols = cols * n_col
    count = contributions.shape[1]
    parts = 4
    table = pltpu.SMEM((1, count), jnp.int32)
    dense, sel = pl.pallas_call(
        spread_kernel,
        out_shape=(shape(slab_cols, rows), shape(PW, PW)),
        in_specs=[HBM_SPEC] * 6,
        out_specs=(VMEM_SPEC,) * 2,
        scratch_shapes=[table] * 3
        + [
            VMEM((count, NB, TR), F32),
            VMEM((cols, rows), F32),
            VMEM((1, PW), jnp.int32),
            DMA((5 + parts,)),
        ],
        compiler_params=pltpu.CompilerParams(vmem_limit_bytes=32 * 1024 * 1024),
    )(*map(stay, (target_column, target_rows, live_rows, contributions, matrix_slab, pivot_index)))
    wide = PW // n_row
    piece = max(8, wide // n_col)
    per = cols // NB
    depth = n_col // 2
    steps = depth * per
    scratch = [
        VMEM((n_row - 1, wide, PW), F32),
        VMEM((wide, PW), F32),
        VMEM((n_col - 1, piece, PW), F32),
        VMEM((PW, PW), F32),
        VMEM((depth - 1, PW // depth, rows), F32),
        VMEM((PW // depth, rows), F32),
        VMEM((PW // depth, rows), F32),
        VMEM((PW // depth, rows), F32),
        VMEM((PW // depth, PW), F32),
        VMEM((steps, NB, rows), F32),
        VMEM((steps, NB, rows), F32),
        VMEM((steps, NB, rows), F32),
        VMEM((cols, rows), F32),
        VMEM((cols, PW), F32),
        VMEM((cols, PW), F32),
        VMEM((per, n_row // 2 - 1, NB, PW), F32),
        VMEM((cols, PW), F32),
        VMEM((rows, PW), F32),
        VMEM((PW, PW), F32),
        VMEM((PW, B), F32),
        VMEM((PW, B), F32),
        VMEM((PW, rows), F32),
        VMEM((cols, PW), F32),
        VMEM((PW, PW), F32),
        VMEM((1, PW), jnp.int32),
        DMA,
        DMA((8,)),
        DMA((4,)),
        DMA((2, n_row)),
        DMA((3, depth)),
        DMA((2, steps)),
        DMA((3, steps)),
        DMA((2, per)),
        DMA((2, per)),
        DMA((3, per)),
    ]
    return pl.pallas_call(
        functools.partial(main_kernel, n_row, n_col),
        out_shape=shape(cols, rows),
        in_specs=[HBM_SPEC] + [VMEM_SPEC] * 2,
        out_specs=VMEM_SPEC,
        scratch_shapes=scratch,
        compiler_params=pltpu.CompilerParams(
            collective_id=0, has_side_effects=True, vmem_limit_bytes=32 * 1024 * 1024
        ),
    )(stay(pivot_index), dense, sel)


def solution(mesh):
    placed = (
        P("pcol", "prow"),
        P("prow", "pcol", None, None),
        P("prow", "pcol"),
        P("prow", "pcol"),
        P("prow", "pcol"),
        P(),
    )
    body = functools.partial(per_device, mesh.shape["prow"], mesh.shape["pcol"])

    def whole(*args):
        return jax.shard_map(
            body, mesh=mesh, in_specs=placed, out_specs=P("pcol", "prow"), check_vma=False
        )(*args)

    return whole
```

```python
import functools

import jax
import jax.numpy as jnp
from jax import lax
from jax.experimental import pallas as pl
from jax.experimental.pallas import tpu as pltpu
from jax.sharding import PartitionSpec as P

PW = 256
NB = 64
TR = 256
B = 64
LAG = 2
AHEAD = 4
EARLY = 3
PACE = 7

HIGHEST = lax.Precision.HIGHEST
VMEM = pltpu.VMEM
F32 = jnp.float32
MESH = pl.DeviceIdType.MESH


def hdot(a, b):
    return jnp.dot(a, b, precision=HIGHEST, preferred_element_type=F32)


def hdot_t(a, b):
    return lax.dot_general(a, b, (((1,), (1,)), ((), ())), precision=HIGHEST, preferred_element_type=F32)


def pick_matrix(pivots, group, rows):
    row = group * rows + lax.broadcasted_iota(jnp.int32, (rows, PW), 0)
    return (row == pivots[...]).astype(F32)


def spread_kernel(tc, tr, lr, blocks, slab, pivots, dense, sel, tcs, trs, lrs, held, own_slab, pivot_row, sem):
    cols, rows = own_slab.shape
    count = held.shape[0]
    parts = sem.shape[0] - 5
    size = count // parts
    tables = [pltpu.make_async_copy(a, b, sem.at[i]) for i, (a, b) in enumerate(((tc, tcs), (tr, trs), (lr, lrs)))]
    rest = pltpu.make_async_copy(slab, own_slab, sem.at[3])
    order = pltpu.make_async_copy(pivots, pivot_row, sem.at[4])
    pieces = [
        pltpu.make_async_copy(
            blocks.at[0, pl.ds(i * size, size)], held.at[pl.ds(i * size, size)], sem.at[5 + i]
        )
        for i in range(parts)
    ]
    for copy in tables + pieces + [rest, order]:
        copy.start()
    dense[...] = jnp.zeros_like(dense)
    lane = lax.broadcasted_iota(jnp.int32, (NB, TR), 1)
    for copy in tables:
        copy.wait()

    def add(index, carry):
        c = pl.multiple_of(tcs[0, index] * NB, NB)
        r = pl.multiple_of(trs[0, index] * TR, TR)
        block = jnp.where(lane < lrs[0, index], held[index], 0.0)
        dense[pl.ds(c, NB), pl.ds(r, TR)] += block
        return carry

    for i in range(parts):
        pieces[i].wait()
        lax.fori_loop(i * size, (i + 1) * size, add, 0)
    rest.wait()
    own = pl.multiple_of(lax.axis_index("pcol") * cols, cols)
    dense[pl.ds(own, cols), :] += own_slab[...]
    order.wait()
    sel[...] = hdot(dense[0:PW, :], pick_matrix(pivot_row, lax.axis_index("prow"), rows))


def eliminate(a, every=4):
    groups = B // 8
    eye = (
        lax.broadcasted_iota(jnp.int32, (B, B), 0) == lax.broadcasted_iota(jnp.int32, (B, B), 1)
    ).astype(F32)
    first = jnp.concatenate([a, eye], axis=1)
    second = jnp.concatenate([a.T, eye], axis=1)
    one = [first[8 * g : 8 * g + 8] for g in range(groups)]
    two = [second[8 * g : 8 * g + 8] for g in range(groups)]
    sub = lax.broadcasted_iota(jnp.int32, (8, 2 * B), 0)
    for k in range(B):
        g0, s0 = divmod(k, 8)
        below = sub > s0
        for which, held in enumerate((one, two)):
            col = jnp.broadcast_to(held[g0][:, k : k + 1], (8, 2 * B))
            scaled = jnp.broadcast_to((held[g0] / col)[s0 : s0 + 1, :], (8, 2 * B))
            for g in range(g0 + 1, groups):
                held[g] = held[g] - held[g][:, k : k + 1] * scaled
            fresh = held[g0] - jnp.where(below, col, 0.0) * scaled
            held[g0] = jnp.where(sub == s0, scaled, fresh) if which == 0 else fresh
        if k % every == every - 1:
            yield None
    first = jnp.concatenate(one, axis=0)
    second = jnp.concatenate(two, axis=0)
    return second[:, :B].T, first[:, :B], first[:, B:], second[:, B:].T


def factor(packed, low_inv, up_inv):
    i = lax.broadcasted_iota(jnp.int32, (B, B), 0)
    j = lax.broadcasted_iota(jnp.int32, (B, B), 1)
    for s in range(0, PW, B):
        e = s + B
        low, up, li, ui = yield from eliminate(packed[s:e, s:e])
        li = jnp.where(i >= j, li, 0.0)
        ui = jnp.where(i <= j, ui, 0.0)
        packed[s:e, s:e] = jnp.where(i >= j, low, up)
        low_inv[s:e, :] = li
        up_inv[s:e, :] = ui
        if e < PW:
            right = hdot(li, packed[s:e, e:])
            left = hdot(packed[e:, s:e], ui)
            packed[s:e, e:] = right
            packed[e:, s:e] = left
            packed[e:, e:] = packed[e:, e:] - hdot(left, right)
        yield None


def main_kernel(
    n_row, n_col,
    pivots, dense, sel, out,
    block_in, block, piece_in, diag, level_in, level_sum, twin_in, band_sum, lead, xr, zl, zr,
    final, mine, pair_in, others, moved, pick, packed, low_inv, up_inv, x, y, inverse,
    pivot_row, pivot_sem, diag_sem, panel_sem, lead_sem, chain_sem, x_sem, z_sem, pair_sem, row_sem, moved_sem,
):
    cols, rows = out.shape
    group, place = lax.axis_index("prow"), lax.axis_index("pcol")
    me = group * n_col + place
    n = n_row * n_col
    owners = PW // cols
    per = cols // NB
    wide = block.shape[0]
    piece = piece_in.shape[1]
    reducers = wide // piece
    pairs = n_row // 2
    depth = n_col // 2
    band = twin_in.shape[0]
    steps = depth * per
    level, side = lax.div(place, 2), lax.rem(place, 2)
    row, core = lax.div(group, 2), lax.rem(group, 2)
    near = depth // 2
    half = lax.div(level, near)
    across = (group, place + 1 - 2 * side)
    partner = (group + 1 - 2 * core, place)

    def local(ref, sem):
        return pltpu.make_async_copy(ref, ref, sem)

    def send(src, dst, ss, rs, where):
        return pltpu.make_async_remote_copy(
            src_ref=src, dst_ref=dst, send_sem=ss, recv_sem=rs, device_id=where, device_id_type=MESH
        )

    def rows_of(ref, start, size):
        return ref.at[pl.ds(pl.multiple_of(start, size), size)]

    pivot_copy = pltpu.make_async_copy(pivots, pivot_row, pivot_sem)
    pivot_copy.start()
    barrier = pltpu.get_barrier_semaphore()

    def greet(d, carry):
        t = lax.rem(me + d, n)
        pl.semaphore_signal(
            barrier, inc=1, device_id=(lax.div(t, n_col), lax.rem(t, n_col)), device_id_type=MESH
        )
        return carry

    lax.fori_loop(1, n, greet, 0)
    pivot_copy.wait()
    pick[...] = pick_matrix(pivot_row, group, rows)
    head = group == 0
    hit = hdot_t(jnp.ones((8, PW), F32), pick[...])[0:1, :] > 0.5
    pl.semaphore_wait(barrier, n - 1)

    for d in range(1, n_row):
        t = lax.rem(group + d, n_row)
        send(rows_of(sel, t * wide, wide), block_in.at[d - 1], diag_sem.at[0], diag_sem.at[1], (t, place)).start()
    def level_send(d):
        t = lax.rem(level + d, depth)
        send(
            rows_of(dense, t * band, band), level_in.at[d - 1], panel_sem.at[0], panel_sem.at[1],
            (group, t * 2 + side),
        ).start()

    def x_where(k):
        zone, c = divmod(k, per)

        def far_goal(i):
            return half * i + (1 - half) * (depth - 1 - i)

        def near_goal(i):
            return half * near + lax.rem(level - half * near + 1 + i, near)

        goal = far_goal(zone) if zone < near else near_goal(zone - near)
        if near == 2 and zone in (1, 2):
            edge = 1 - lax.rem(lax.div(level + 1, 2), 2)
            goal = edge * goal + (1 - edge) * (near_goal(0) if zone == 1 else far_goal(1))
        return goal, c

    def x_copy(k):
        goal, c = x_where(k)
        owner = goal * 2 + 1 - side
        src = rows_of(dense, owner * cols + c * NB, NB)
        return owner >= owners, send(src, xr.at[k], x_sem.at[0, k], x_sem.at[1, k], across)

    def x_send(k):
        if k < steps:
            live, copy = x_copy(k)
            pl.when(live)(copy.start)

    def if_reducer(f):
        if reducers == n_col:
            f()
        else:
            pl.when(place < reducers)(f)

    def if_not_reducer(f):
        if reducers != n_col:
            pl.when(place >= reducers)(f)

    level_send(1)
    x_send(0)
    local(block_in, diag_sem.at[1]).wait()
    at = pl.multiple_of(group * wide, wide)
    block[...] = sel[pl.ds(at, wide), :] + jnp.sum(block_in[...], axis=0)

    def piece_send(d, carry):
        t = lax.rem(place + d, n_col)

        def go():
            send(
                rows_of(block, t * piece, piece), piece_in.at[d - 1], diag_sem.at[2], diag_sem.at[3], (group, t)
            ).start()

        if reducers == n_col:
            go()
        else:
            pl.when(t < reducers)(go)
        return carry

    lax.fori_loop(1, n_col, piece_send, 0)
    level_send(depth - 1)
    x_send(1)
    own_band = pl.multiple_of(level * band, band)

    def twin_copy():
        return send(level_sum, twin_in, panel_sem.at[2], panel_sem.at[3], across)

    def panel_sum():
        local(level_in, panel_sem.at[1]).wait()
        level_sum[...] = dense[pl.ds(own_band, band), :] + jnp.sum(level_in[...], axis=0)
        twin_copy().start()

    def lead_copy(d):
        return send(
            band_sum.at[:, 0:PW], lead, lead_sem.at[0, d], lead_sem.at[1, 0], (lax.rem(group + d, n_row), place)
        )

    def panel_twin():
        twin_copy().wait_recv()
        band_sum[...] = level_sum[...] + twin_in[...]

        @pl.when(group == 0)
        def _():
            for d in range(1, n_row):
                lead_copy(d).start()

    def chain_copy(index, way):
        own = rows_of(x, index * band, band)
        return send(
            own, own, chain_sem.at[0 if way > 0 else 1, index], chain_sem.at[2, index], (group, place + 2 * way)
        )

    def panel_swap():
        @pl.when(group > 0)
        def _():
            local(lead, lead_sem.at[1, 0]).wait()

        @pl.when(group == 0)
        def _():
            lead[...] = band_sum[:, 0:PW]

        x[pl.ds(own_band, band), :] = jnp.where(hit, hdot_t(lead[...], pick[...]), band_sum[...])
        pl.when(level < depth - 1)(chain_copy(level, 1).start)
        pl.when(level > 0)(chain_copy(level, -1).start)

    def panel_step(s, way, final_stop):
        index = level - s * way
        inside = (index >= 0) & (index < depth)
        index = lax.rem(index + depth, depth)
        end = (level == depth - 1) if way > 0 else (level == 0)

        @pl.when(inside & (end if final_stop else jnp.logical_not(end)))
        def _():
            chain_copy(index, way).wait_recv()
            if not final_stop:
                chain_copy(index, way).start()

    def panel_stage(s):
        for way in (1, -1):
            panel_step(s, way, False)

    def panel_collect():
        for s in range(1, depth):
            for way in (1, -1):
                panel_step(s, way, True)

    def panel_sent():
        for b in range(depth):
            pl.when((b <= level) & (level < depth - 1))(chain_copy(b, 1).wait_send)
            pl.when((b >= level) & (level > 0))(chain_copy(b, -1).wait_send)

    diag_at = pl.multiple_of(group * wide + place * piece, piece)

    @if_reducer
    def _():
        local(piece_in, diag_sem.at[3]).wait()
        mid = pl.multiple_of(place * piece, piece)
        diag[pl.ds(diag_at, piece), :] = block[pl.ds(mid, piece), :] + jnp.sum(piece_in[...], axis=0)

        def piece_spread(d, carry):
            own = diag.at[pl.ds(diag_at, piece)]
            send(own, own, diag_sem.at[4], diag_sem.at[5], (group, lax.rem(place + d, n_col))).start()
            return carry

        lax.fori_loop(1, n_col, piece_spread, 0)

    for d in range(2, depth - 1):
        level_send(d)
    x_send(2)
    x_send(3)

    def z_copy(k, way):
        goal, c = x_where(k)
        slot = goal * per + c
        into = zl if way > 0 else zr
        return send(
            xr.at[k], into.at[slot], z_sem.at[0, slot], z_sem.at[1 if way > 0 else 2, slot], (group, place + 2 * way)
        )

    def pair_copy(c):
        return send(mine.at[pl.ds(c * NB, NB)], pair_in.at[pl.ds(c * NB, NB)], pair_sem.at[0, c], pair_sem.at[1, c], partner)

    def moved_pair(c):
        return send(
            final.at[pl.ds(c * NB, NB), 0:PW], moved.at[pl.ds(c * NB, NB)], moved_sem.at[0, c], moved_sem.at[1, c],
            partner,
        )

    def moved_pass(c):
        into = moved.at[pl.ds(c * NB, NB)]
        return send(into, into, moved_sem.at[0, c], moved_sem.at[1, c], partner)

    def row_copy(c, d):
        where = (lax.rem(row + d, pairs) * 2 + core, place)
        return send(
            pair_in.at[pl.ds(c * NB, NB)], others.at[c, d - 1], row_sem.at[0, c], row_sem.at[1, c], where
        )

    def moved_copy(c, d):
        where = (lax.rem(row + d, pairs) * 2 + core, place)
        into = moved.at[pl.ds(c * NB, NB)]
        return send(into, into, moved_sem.at[2, c], moved_sem.at[1, c], where)

    def goal_of(k):
        goal, c = x_where(k)
        return goal, c, goal * 2 + side, goal * per + c

    def x_part(k):
        goal, c, owner, slot = goal_of(k)

        @pl.when(owner >= owners)
        def _():
            x_copy(k)[1].wait_recv()
            at = pl.multiple_of(owner * cols + c * NB, NB)
            xr[k] = xr[k] + dense[pl.ds(at, NB), :]

            @pl.when((level < goal) & (level == 0))
            def _():
                z_copy(k, 1).start()

            @pl.when((level > goal) & (level == depth - 1))
            def _():
                z_copy(k, -1).start()

    def z_part(k):
        goal, c, owner, slot = goal_of(k)

        @pl.when(owner >= owners)
        def _():
            @pl.when((level <= goal) & (level > 0))
            def _():
                pltpu.make_async_copy(zl.at[slot], zl.at[slot], z_sem.at[1, slot]).wait()
                xr[k] = xr[k] + zl[slot]

            @pl.when((level >= goal) & (level < depth - 1))
            def _():
                pltpu.make_async_copy(zr.at[slot], zr.at[slot], z_sem.at[2, slot]).wait()
                xr[k] = xr[k] + zr[slot]

            @pl.when((level < goal) & (level > 0))
            def _():
                z_copy(k, 1).start()

            @pl.when((level > goal) & (level < depth - 1))
            def _():
                z_copy(k, -1).start()

            if k >= steps - per:
                final[c * NB : c * NB + NB, :] = xr[k]
                mine[c * NB : c * NB + NB, :] = hdot(xr[k], pick[...])
                pair_copy(c).start()
                pl.when(group == 0)(moved_pair(c).start)

    def row_part(c):
        @pl.when(place >= owners)
        def _():
            lo = c * NB
            pair_copy(c).wait()
            pair_in[lo : lo + NB, :] = pair_in[lo : lo + NB, :] + mine[lo : lo + NB, :]
            for d in range(1, pairs):
                row_copy(c, d).start()

            @pl.when(group == 0)
            def _():
                moved[lo : lo + NB, :] = final[lo : lo + NB, 0:PW]

            @pl.when(group == 1)
            def _():
                local(moved.at[pl.ds(lo, NB)], moved_sem.at[1, c]).wait()

            @pl.when(group == 0)
            def _():
                for d in range(1, pairs):
                    moved_copy(c, d).start()

    x_part(0)
    kept = (reducers - 1) * piece
    local(diag.at[pl.ds(0, kept)], diag_sem.at[5]).wait()
    if_not_reducer(lambda: local(diag.at[pl.ds(0, piece)], diag_sem.at[5]).wait())
    for d in range(1, n_row):
        own = rows_of(diag, group * wide, wide)
        send(own, own, diag_sem.at[6], diag_sem.at[7], (lax.rem(group + d, n_row), place)).start()
    for k in range(4, AHEAD + 1):
        x_send(k)
    for k in range(1, EARLY):
        x_part(k)
    local(diag.at[pl.ds(0, (n_row - 1) * wide)], diag_sem.at[7]).wait()
    packed[...] = diag[...]

    def all_work():
        yield from factor(packed, low_inv, up_inv)
        inverse[...] = jnp.zeros_like(inverse)
        for s in range(0, PW, B):
            e = s + B
            inverse[s:e, s:e] = up_inv[s:e, :]
            if s:
                term = hdot(packed[0:s, s:e], up_inv[s:e, :])
                inverse[0:s, s:e] = -hdot(inverse[0:s, 0:s], term)
            yield None

    work = all_work()

    def solve_x():
        panel_collect()
        panel_sent()
        x[:, 0:PW] = jnp.where(head, diag[...], x[:, 0:PW])
        for s in range(0, PW, B):
            e = s + B
            term = x[s:e, :]
            if s:
                term = term - hdot(packed[s:e, 0:s], x[0:s, :])
            x[s:e, :] = hdot(low_inv[s:e, :], term)

    def finish(begin, end):
        @pl.when(place >= owners)
        def _():
            for c in range(begin, end):
                lo = c * NB
                local(others.at[c], row_sem.at[1, c]).wait()

                @pl.when(row > 0)
                def _():
                    local(moved.at[pl.ds(lo, NB)], moved_sem.at[1, c]).wait()
                    pl.when(core == 0)(moved_pass(c).start)

                mine[lo : lo + NB, :] = pair_in[lo : lo + NB, :] + jnp.sum(others[c], axis=0)
            lo, hi = begin * NB, end * NB
            y[lo:hi, :] = hdot(mine[lo:hi, :], inverse[...])
            swapped = jnp.where(hit, hdot_t(moved[lo:hi, :], pick[...]), final[lo:hi, :])
            out[lo:hi, :] = swapped - hdot(y[lo:hi, :], x[...])
            out[lo:hi, 0:PW] = jnp.where(head, y[lo:hi, :], out[lo:hi, 0:PW])

    far = near * per
    last = steps - per
    for k in range(1, steps):
        for s in range(1, depth - 1):
            if k == (4 + 2 * s if near == 2 else 5):
                panel_stage(s)
        if k >= EARLY:
            x_part(k)
        if 0 <= k - LAG < far:
            z_part(k - LAG)
        if k >= far:
            z_part(k)
        if k == 1:
            panel_sum()
            for later in range(AHEAD + 1, steps):
                x_send(later)
        if k == 3:
            panel_twin()
        if k == 4:
            panel_swap()
        for _ in range(PACE):
            next(work, None)
        if k == min(last + 1, steps - 1):
            for _ in work:
                pass
            solve_x()
        if k > last:
            row_part(k - last - 1)
        if k > last + 2:
            finish(k - last - 3, k - last - 2)
    row_part(per - 1)
    for c in range(max(per - 3, 0), per):
        finish(c, c + 1)

    @pl.when(place < owners)
    def _():
        x[:, 0:PW] = jnp.where(head, packed[...], x[:, 0:PW])
        off = pl.multiple_of(lax.rem(place, owners) * cols, cols)
        out[...] = x[pl.ds(off, cols), :]

    local(block_in, diag_sem.at[0]).wait()
    local(block.at[pl.ds(0, kept)], diag_sem.at[2]).wait()
    if_not_reducer(lambda: local(block.at[pl.ds(0, piece)], diag_sem.at[2]).wait())
    if_reducer(lambda: local(piece_in, diag_sem.at[4]).wait())
    local(block_in, diag_sem.at[6]).wait()
    local(level_in, panel_sem.at[0]).wait()
    twin_copy().wait_send()

    @pl.when(group == 0)
    def _():
        for d in range(1, n_row):
            lead_copy(d).wait_send()

    for k in range(steps):
        live, copy = x_copy(k)
        pl.when(live)(copy.wait_send)
        goal, c, owner, slot = goal_of(k)

        @pl.when((owner >= owners) & (level != goal))
        def _():
            z_copy(k, 1).wait_send()

    @pl.when(place >= owners)
    def _():
        for c in range(per):
            local(others.at[c], row_sem.at[0, c]).wait()
            pl.when(core == 0)(moved_pair(c).wait_send)

            @pl.when(group == 0)
            def _():
                local(others.at[c], moved_sem.at[2, c]).wait()


def stay(array):
    return pltpu.with_memory_space_constraint(array, pltpu.MemorySpace.HBM)


def shape(*dims):
    return jax.ShapeDtypeStruct(dims, F32)


HBM_SPEC = pl.BlockSpec(memory_space=pltpu.MemorySpace.HBM)
VMEM_SPEC = pl.BlockSpec(memory_space=pltpu.VMEM)
DMA = pltpu.SemaphoreType.DMA


def per_device(
    n_row, n_col, matrix_slab, contributions, target_column, target_rows, live_rows, pivot_index
):
    cols, rows = matrix_slab.shape
    slab_cols = cols * n_col
    count = contributions.shape[1]
    parts = 4
    table = pltpu.SMEM((1, count), jnp.int32)
    dense, sel = pl.pallas_call(
        spread_kernel,
        out_shape=(shape(slab_cols, rows), shape(PW, PW)),
        in_specs=[HBM_SPEC] * 6,
        out_specs=(VMEM_SPEC,) * 2,
        scratch_shapes=[table] * 3
        + [
            VMEM((count, NB, TR), F32),
            VMEM((cols, rows), F32),
            VMEM((1, PW), jnp.int32),
            DMA((5 + parts,)),
        ],
        compiler_params=pltpu.CompilerParams(vmem_limit_bytes=32 * 1024 * 1024),
    )(*map(stay, (target_column, target_rows, live_rows, contributions, matrix_slab, pivot_index)))
    wide = PW // n_row
    piece = max(8, wide // n_col)
    per = cols // NB
    depth = n_col // 2
    steps = depth * per
    scratch = [
        VMEM((n_row - 1, wide, PW), F32),
        VMEM((wide, PW), F32),
        VMEM((n_col - 1, piece, PW), F32),
        VMEM((PW, PW), F32),
        VMEM((depth - 1, PW // depth, rows), F32),
        VMEM((PW // depth, rows), F32),
        VMEM((PW // depth, rows), F32),
        VMEM((PW // depth, rows), F32),
        VMEM((PW // depth, PW), F32),
        VMEM((steps, NB, rows), F32),
        VMEM((steps, NB, rows), F32),
        VMEM((steps, NB, rows), F32),
        VMEM((cols, rows), F32),
        VMEM((cols, PW), F32),
        VMEM((cols, PW), F32),
        VMEM((per, n_row // 2 - 1, NB, PW), F32),
        VMEM((cols, PW), F32),
        VMEM((rows, PW), F32),
        VMEM((PW, PW), F32),
        VMEM((PW, B), F32),
        VMEM((PW, B), F32),
        VMEM((PW, rows), F32),
        VMEM((cols, PW), F32),
        VMEM((PW, PW), F32),
        VMEM((1, PW), jnp.int32),
        DMA,
        DMA((8,)),
        DMA((4,)),
        DMA((2, n_row)),
        DMA((3, depth)),
        DMA((2, steps)),
        DMA((3, steps)),
        DMA((2, per)),
        DMA((2, per)),
        DMA((3, per)),
    ]
    return pl.pallas_call(
        functools.partial(main_kernel, n_row, n_col),
        out_shape=shape(cols, rows),
        in_specs=[HBM_SPEC] + [VMEM_SPEC] * 2,
        out_specs=VMEM_SPEC,
        scratch_shapes=scratch,
        compiler_params=pltpu.CompilerParams(
            collective_id=0, has_side_effects=True, vmem_limit_bytes=32 * 1024 * 1024
        ),
    )(stay(pivot_index), dense, sel)


def solution(mesh):
    placed = (
        P("pcol", "prow"),
        P("prow", "pcol", None, None),
        P("prow", "pcol"),
        P("prow", "pcol"),
        P("prow", "pcol"),
        P(),
    )
    body = functools.partial(per_device, mesh.shape["prow"], mesh.shape["pcol"])

    def whole(*args):
        return jax.shard_map(
            body, mesh=mesh, in_specs=placed, out_specs=P("pcol", "prow"), check_vma=False
        )(*args)

    return whole
```
